128 devices in a mesh: case: 1, ens: 128 (over z, y, x, core).
Axes of the slice: x: 4, y: 4, z: 4, core: 2. Of those that a mesh axis runs over, the one named last changes fastest.
Arguments:
- x_init: float32 [128, 512, 69], P(('case', 'ens'))
- a_mix: bfloat16 [512, 512], replicated
- w_in: bfloat16 [4, 69, 512], replicated
- w_out: bfloat16 [4, 512, 69], replicated
- y_obs: float32 [8, 512, 8], P(None, ('case', 'ens'))
- r_inv: float32 [512, 7, 8], P(('case', 'ens'))
- obs_idx: int32 [8], replicated
Outputs:
- output: float32 [128, 512, 69], P(('case', 'ens'))
All inputs are finite; a program needn't handle non-finite values.
Results may differ from the reference program's by a relative error of at most 0.00935664.
Values are sent between devices in bfloat16 or wider.
A program may use at most 1 GiB of HBM per device.

```python
import math
import functools
import jax
import jax.numpy as jnp
from jax import lax

MEMBERS = 128
COLS = 512
VARS = 69
HIDDEN = 512
OBS_VARS = 8
NS_STEPS = 16
HALO = 3
LAYERS = 4
CYCLES = 8
COL_BLOCK = 4

LOC_COLS = 2 * HALO + 1


def setup_inputs(seed: int = 0, part: int = 0) -> dict:
    base_key = jax.random.key(seed)
    shared_keys = jax.random.split(base_key, 4)
    part_keys = jax.random.split(jax.random.fold_in(base_key, part), 6)
    a_mix = jax.random.normal(shared_keys[0], (COLS, COLS), jnp.float32) / math.sqrt(COLS)
    w_in = jax.random.normal(shared_keys[1], (LAYERS, VARS, HIDDEN), jnp.float32) / math.sqrt(VARS)
    out_scale = 0.8 / math.sqrt(HIDDEN * LAYERS * CYCLES)
    w_out = out_scale * jax.random.normal(shared_keys[2], (LAYERS, HIDDEN, VARS), jnp.float32)
    obs_idx = jax.random.permutation(shared_keys[3], VARS)[:OBS_VARS].astype(jnp.int32)
    background = jax.random.normal(part_keys[0], (COLS, VARS), jnp.float32)
    member_amp = jax.random.normal(part_keys[1], (MEMBERS, COLS), jnp.float32)
    pattern = jax.random.normal(part_keys[2], (COLS, VARS), jnp.float32)
    noise = jax.random.normal(part_keys[3], (MEMBERS, COLS, VARS), jnp.float32)
    x_init = background[None] + 0.4 * member_amp[:, :, None] * pattern[None] + 0.25 * noise
    obs_noise = jax.random.normal(part_keys[4], (CYCLES, COLS, OBS_VARS), jnp.float32)
    y_obs = jnp.take(background, obs_idx, axis=1)[None] + 0.6 * obs_noise
    root_sum = math.sqrt(LOC_COLS * OBS_VARS) + math.sqrt(MEMBERS)
    obs_scale = 6.0 * (MEMBERS - 1) / (root_sum * root_sum)
    scaled = (jnp.arange(LOC_COLS, dtype=jnp.float32) - HALO) / HALO
    loc_taper = jnp.exp(-0.5 * scaled * scaled)
    spread_draw = jax.random.uniform(part_keys[5], (COLS, LOC_COLS, OBS_VARS), jnp.float32, 0.25, 1.75)
    r_inv = obs_scale * loc_taper[None, :, None] * spread_draw
    return {'x_init': x_init, 'a_mix': a_mix.astype(jnp.bfloat16), 'w_in': w_in.astype(jnp.bfloat16), 'w_out': w_out.astype(jnp.bfloat16), 'y_obs': y_obs, 'r_inv': r_inv, 'obs_idx': obs_idx}


def member_forecast(member, a_mix, w_in, w_out):
    def layer_step(state, layer_w):
        w_first, w_second = layer_w
        mixed = jnp.dot(a_mix, state.astype(jnp.bfloat16), preferred_element_type=jnp.float32).astype(jnp.bfloat16)
        hidden = jnp.dot(mixed, w_first, preferred_element_type=jnp.float32)
        hidden_act = jax.nn.gelu(hidden, approximate=True).astype(jnp.bfloat16)
        return state + jnp.dot(hidden_act, w_second, preferred_element_type=jnp.float32), None
    member, _ = lax.scan(layer_step, member, (w_in, w_out))
    return member


def analysis_weights(win_pert, win_wt, win_innov):
    identity = jnp.eye(MEMBERS, dtype=jnp.float32)
    weighted = win_pert * win_wt[:, :, None, :]
    gram = jnp.einsum('bokp,bolp->bkl', weighted, win_pert)
    drive = jnp.einsum('bokp,bop->bk', weighted, win_innov)
    precision_mat = (MEMBERS - 1) / 1.2 * identity + gram
    trace_val = jnp.trace(precision_mat, axis1=1, axis2=2)
    def ns_step(index, carry):
        iter_y, iter_z = carry
        factor = 0.5 * (3.0 * identity - jnp.einsum('bij,bjk->bik', iter_z, iter_y))
        return jnp.einsum('bij,bjk->bik', iter_y, factor), jnp.einsum('bij,bjk->bik', factor, iter_z)
    start_pair = (precision_mat / trace_val[:, None, None], jnp.broadcast_to(identity, precision_mat.shape))
    iter_y, iter_z = lax.fori_loop(0, NS_STEPS, ns_step, start_pair)
    inv_root = iter_z / jnp.sqrt(trace_val)[:, None, None]
    mean_w = jnp.einsum('bij,bj->bi', inv_root, jnp.einsum('bij,bj->bi', inv_root, drive))
    return math.sqrt(MEMBERS - 1) * inv_root + mean_w[:, :, None]


def analysis(col_state, obs_now, r_inv, obs_idx):
    ens_mean = jnp.mean(col_state, axis=1)
    pert = col_state - ens_mean[:, None, :]
    obs_pert = jnp.take(pert, obs_idx, axis=2)
    innovation = obs_now - jnp.take(ens_mean, obs_idx, axis=1)
    pack = jnp.concatenate([obs_pert, innovation[:, None, :]], axis=1)
    extended = jnp.concatenate([pack[COLS - HALO:], pack, pack[:HALO]], axis=0)
    def block_step(start):
        window = jnp.stack([lax.dynamic_slice_in_dim(extended, start + offset, COL_BLOCK, axis=0) for offset in range(LOC_COLS)], axis=1)
        win_wt = lax.dynamic_slice_in_dim(r_inv, start, COL_BLOCK, axis=0)
        blk_pert = lax.dynamic_slice_in_dim(pert, start, COL_BLOCK, axis=0)
        blk_mean = lax.dynamic_slice_in_dim(ens_mean, start, COL_BLOCK, axis=0)
        weights = analysis_weights(window[:, :, :MEMBERS], win_wt, window[:, :, MEMBERS])
        return blk_mean[:, None, :] + jnp.einsum('bik,biv->bkv', weights, blk_pert)
    starts = jnp.arange(COLS // COL_BLOCK) * COL_BLOCK
    return lax.map(block_step, starts).reshape(COLS, MEMBERS, VARS)


def reference(x_init, a_mix, w_in, w_out, y_obs, r_inv, obs_idx):
    step_member = functools.partial(member_forecast, a_mix=a_mix, w_in=w_in, w_out=w_out)
    def cycle_step(ensemble, obs_now):
        forecast_ens = lax.map(step_member, ensemble)
        analysed = analysis(jnp.transpose(forecast_ens, (1, 0, 2)), obs_now, r_inv, obs_idx)
        return jnp.transpose(analysed, (1, 0, 2)), None
    final, _ = lax.scan(cycle_step, x_init, y_obs)
    return final
```

```python
import functools
import math
import jax
import jax.numpy as jnp
from jax import lax
from jax.experimental import pallas as pl
from jax.experimental.pallas import tpu as pltpu
from jax.sharding import PartitionSpec as P

INFLATION = 1.2
NS_STEPS = 16
FULL = lax.Precision.HIGHEST
MESH = pl.DeviceIdType.MESH
BF16 = jnp.bfloat16
F32 = jnp.float32
LANES = 128
PREV_LANE = 72
NEXT_LANE = 96
GAIN_LANE = 127


def split3(x):
    hi = x.astype(BF16)
    rest = x - hi.astype(F32)
    mid = rest.astype(BF16)
    lo = (rest - mid.astype(F32)).astype(BF16)
    return hi, mid, lo


def lhs_pack(x):
    hi, mid, lo = split3(x)
    return jnp.concatenate([hi, mid, hi, mid, hi, lo], axis=1)


def rhs_pack(x):
    hi, mid, lo = split3(x)
    return jnp.concatenate([hi, hi, mid, mid, lo, hi], axis=0)


def dot32(lhs, rhs):
    return jnp.dot(lhs, rhs, preferred_element_type=F32)


def kernel(num_dev, num_cycles, num_obs, halo,
           obs_ref, x_ref, a_ref, win_ref, wout_ref, y_ref, r_ref,
           out_ref,
           state, win_s, wout_s, send1, land1, send2, land2, xz, yprev, ynext, yall,
           s1, r1, s2, r2, sy0, ry0, sy1, ry1):
    me = lax.axis_index('ens')
    num_cols, num_vars = x_ref.shape
    num_layers = win_ref.shape[0]
    blk = num_cols // num_dev
    num_mem = num_dev

    bar = pltpu.get_barrier_semaphore()
    def greet(i, carry):
        pl.semaphore_signal(bar, inc=1, device_id={'ens': lax.rem(me + i, num_dev)}, device_id_type=MESH)
        return carry
    lax.fori_loop(1, num_dev, greet, 0)

    var = lax.broadcasted_iota(jnp.int32, (LANES, LANES), 0)
    lane = lax.broadcasted_iota(jnp.int32, (LANES, LANES), 1)
    place = var + num_obs
    for i in range(num_obs):
        place = place - jnp.where(var > obs_ref[i], 1, 0)
    for i in range(num_obs):
        place = jnp.where(var == obs_ref[i], i, place)
    to_lane = jnp.where((place == lane) & (var < num_vars), 1.0, 0.0).astype(F32)
    to_lane_b = to_lane.astype(BF16)
    eye = jnp.where(var == lane, 1.0, 0.0).astype(F32)

    state[...] = jnp.dot(x_ref[...], to_lane[:num_vars], precision=FULL, preferred_element_type=F32)
    for l in range(num_layers):
        win_s[l] = lax.dot_general(to_lane_b[:num_vars], win_ref[l], (((0,), (0,)), ((), ())),
                                   preferred_element_type=F32).astype(BF16)
        wout_s[l] = jnp.dot(wout_ref[l], to_lane_b[:num_vars], preferred_element_type=F32).astype(BF16)

    send1_rows = send1.reshape(num_cols, LANES)
    land1_rows = land1.reshape(num_mem * blk, LANES)
    send2_rows = send2.reshape(num_mem * blk, LANES)
    land2_rows = land2.reshape(num_cols, LANES)

    def scatter(src, dst, ss, rs):
        def body(i, carry):
            peer = lax.rem(me + i, num_dev)
            pltpu.make_async_remote_copy(src_ref=src.at[peer], dst_ref=dst.at[me], send_sem=ss, recv_sem=rs,
                                         device_id={'ens': peer}, device_id_type=MESH).start()
            return carry
        lax.fori_loop(1, num_dev, body, 0)
        dst[pl.ds(me, 1)] = src[pl.ds(me, 1)]

    def settle(src, dst, ss, rs):
        pltpu.make_async_copy(src.at[pl.ds(0, num_dev - 1)], dst.at[pl.ds(0, num_dev - 1)], ss).wait()
        pltpu.make_async_copy(src.at[pl.ds(0, num_dev - 1)], dst.at[pl.ds(0, num_dev - 1)], rs).wait()

    def y_copies():
        right = lax.rem(me + 1, num_dev)
        left = lax.rem(me + num_dev - 1, num_dev)
        return (pltpu.make_async_remote_copy(src_ref=y_ref, dst_ref=yprev, send_sem=sy0, recv_sem=ry0,
                                             device_id={'ens': right}, device_id_type=MESH),
                pltpu.make_async_remote_copy(src_ref=y_ref, dst_ref=ynext, send_sem=sy1, recv_sem=ry1,
                                             device_id={'ens': left}, device_id_type=MESH))

    TILE = 128
    def forecast():
        for l in range(num_layers):
            hb = state[...].astype(BF16)
            for t in range(num_cols // TILE):
                rows = pl.ds(t * TILE, TILE)
                mixed = jnp.dot(a_ref[rows, :], hb, preferred_element_type=F32).astype(BF16)
                hidden = jnp.dot(mixed, win_s[l], preferred_element_type=F32)
                act = jax.nn.gelu(hidden, approximate=True).astype(BF16)
                state[rows, :] += jnp.dot(act, wout_s[l], preferred_element_type=F32)

    lane_row = lax.broadcasted_iota(jnp.int32, (num_cols, LANES), 1)
    col_row = lax.broadcasted_iota(jnp.int32, (num_cols, LANES), 0) % blk

    def pack_state():
        h = state[...]
        before = pltpu.roll(h, blk, 0)
        after = pltpu.roll(h, num_cols - blk, 0)
        res = h
        for n in range(2 * halo):
            if n < halo:
                col, src, lane0 = (n - halo) % blk, before, PREV_LANE + n * num_obs
            else:
                col, src, lane0 = n - halo, after, NEXT_LANE + (n - halo) * num_obs
            moved = pltpu.roll(src, lane0, 1)
            here = (lane_row >= lane0) & (lane_row < lane0 + num_obs)
            res = jnp.where(here, jnp.where(col_row == col, moved, 0.0), res)
        send1_rows[...] = res

    mem_lane = lax.broadcasted_iota(jnp.int32, (num_mem, LANES), 1)

    def analyse(cycle):
        raws = [land1_rows[pl.ds(j, num_mem, stride=blk), :] for j in range(blk)]
        halo_sum = raws[0]
        for j in range(1, blk):
            halo_sum = halo_sum + raws[j]
        own = raws[0]
        for j in range(1, blk):
            own = jnp.where(mem_lane >= j * num_obs, pltpu.roll(raws[j], j * num_obs, 1), own)
        obs_raw = jnp.where(mem_lane < blk * num_obs, own, halo_sum)
        unused = ((mem_lane >= blk * num_obs) & (mem_lane < PREV_LANE)) | (mem_lane >= NEXT_LANE + halo * num_obs)
        obs_raw = jnp.where(unused, 0.0, obs_raw)
        obs_mean = jnp.mean(obs_raw, axis=0, keepdims=True)
        pert = obs_raw - obs_mean
        innov = yall[pl.ds(cycle, 1), :] - obs_mean
        r_all = r_ref[...]
        energy = jnp.sum(pert * pert, axis=0, keepdims=True)
        base = (num_mem - 1) / INFLATION
        trace = num_mem * base + jnp.sum(r_all * energy, axis=1, keepdims=True)
        innov_rows = jnp.where(lax.broadcasted_iota(jnp.int32, (LANES, LANES), 0) == GAIN_LANE, innov, 0.0)
        right = jnp.concatenate([pert, innov_rows], axis=0)
        means = []
        for j in range(blk):
            weighted = pert * r_all[j:j + 1]
            res = lax.dot_general(weighted, right, (((1,), (1,)), ((), ())), precision=FULL, preferred_element_type=F32)
            inv = 1.0 / trace[j:j + 1]
            xz[j, :, :LANES] = (res[:, :LANES] + base * eye) * inv
            mean = jnp.mean(raws[j], axis=0, keepdims=True)
            means.append(mean)
            xz[j, :, LANES:] = jnp.where(mem_lane < num_vars, raws[j] - mean, res[:, LANES:])

        def ns_step(k, carry):
            for j in range(blk):
                both = xz[j]
                factor = 1.5 * eye - 0.5 * both[:, :LANES]
                lhs = lhs_pack(factor)
                first = dot32(lhs, rhs_pack(both))
                xz[j, :, LANES:] = first[:, LANES:]
                xz[j, :, :LANES] = dot32(lhs, rhs_pack(first[:, :LANES]))
            return carry
        lax.fori_loop(0, NS_STEPS - 1, ns_step, 0)

        for j in range(blk):
            factor = 1.5 * eye - 0.5 * xz[j, :, :LANES]
            fin = dot32(lhs_pack(factor), rhs_pack(xz[j, :, LANES:]))
            inv = 1.0 / trace[j:j + 1]
            shift = jnp.sum(fin * fin[:, GAIN_LANE:GAIN_LANE + 1], axis=0, keepdims=True) * inv
            new = means[j] + shift + (math.sqrt(num_mem - 1) * jnp.sqrt(inv)) * fin
            send2_rows[pl.ds(j, num_mem, stride=blk), :] = jnp.where(mem_lane < num_vars, new, 0.0)

    def cycle_body(cycle, carry):
        forecast()
        pack_state()
        @pl.when(cycle == 0)
        def _():
            pl.semaphore_wait(bar, num_dev - 1)
            for copy in y_copies():
                copy.start()
        scatter(send1, land1, s1, r1)
        @pl.when(cycle == 0)
        def _():
            for copy in y_copies():
                copy.wait()
            ylane = lax.broadcasted_iota(jnp.int32, (num_cycles, LANES), 1)
            width = halo * num_obs
            prev = pltpu.roll(yprev[...], PREV_LANE - (blk - halo) * num_obs, 1)
            nxt = pltpu.roll(ynext[...], NEXT_LANE, 1)
            full = y_ref[...]
            full = jnp.where((ylane >= PREV_LANE) & (ylane < PREV_LANE + width), prev, full)
            full = jnp.where((ylane >= NEXT_LANE) & (ylane < NEXT_LANE + width), nxt, full)
            yall[...] = full
        settle(send1, land1, s1, r1)
        analyse(cycle)
        scatter(send2, land2, s2, r2)
        settle(send2, land2, s2, r2)
        state[...] = land2_rows[...]
        return carry
    lax.fori_loop(0, num_cycles, cycle_body, 0)

    final = lax.dot_general(state[...], to_lane, (((1,), (1,)), ((), ())), precision=FULL, preferred_element_type=F32)
    out_ref[...] = final[:, :num_vars]


def solution(mesh):
    num_dev = mesh.shape['ens']

    def local_run(x_blk, a_mix, w_in, w_out, y_blk, r_blk, obs_idx):
        _, num_cols, num_vars = x_blk.shape
        num_cycles, blk, num_obs = y_blk.shape
        halo = (r_blk.shape[1] - 1) // 2
        num_layers, _, num_hid = w_in.shape
        y_flat = jnp.pad(y_blk.reshape(num_cycles, blk * num_obs), ((0, 0), (0, LANES - blk * num_obs)))
        spread = jnp.stack([jnp.pad(r_blk[j], ((j, blk - 1 - j), (0, 0))) for j in range(blk)])
        spread = spread.reshape(blk, (blk + 2 * halo) * num_obs)
        width = halo * num_obs
        prev, own, nxt = spread[:, :width], spread[:, width:width + blk * num_obs], spread[:, width + blk * num_obs:]
        r_all = jnp.concatenate([
            own, jnp.zeros((blk, PREV_LANE - blk * num_obs), F32), prev,
            jnp.zeros((blk, NEXT_LANE - PREV_LANE - width), F32), nxt,
            jnp.zeros((blk, LANES - NEXT_LANE - width), F32)], axis=1)
        vmem = pl.BlockSpec(memory_space=pltpu.VMEM)
        block = pltpu.VMEM((num_dev, blk, LANES), F32)
        out = pl.pallas_call(
            functools.partial(kernel, num_dev, num_cycles, num_obs, halo),
            out_shape=jax.ShapeDtypeStruct((num_cols, num_vars), F32),
            in_specs=[pl.BlockSpec(memory_space=pltpu.SMEM)] + [vmem] * 6,
            out_specs=vmem,
            scratch_shapes=[
                pltpu.VMEM((num_cols, LANES), F32),
                pltpu.VMEM((num_layers, LANES, num_hid), BF16),
                pltpu.VMEM((num_layers, num_hid, LANES), BF16),
                block, block, block, block,
                pltpu.VMEM((blk, num_dev, 2 * LANES), F32),
                pltpu.VMEM((num_cycles, LANES), F32),
                pltpu.VMEM((num_cycles, LANES), F32),
                pltpu.VMEM((num_cycles, LANES), F32),
            ] + [pltpu.SemaphoreType.DMA] * 8,
            compiler_params=pltpu.CompilerParams(collective_id=0, has_side_effects=True),
        )(obs_idx, x_blk[0], a_mix, w_in, w_out, y_flat, r_all)
        return out[None]

    row_spec = P(('case', 'ens'), None, None)
    return jax.shard_map(local_run, mesh=mesh,
                         in_specs=(row_spec, P(), P(), P(), P(None, ('case', 'ens'), None), row_spec, P()),
                         out_specs=row_spec, check_vma=False)
```

```python
import functools
import math
import jax
import jax.numpy as jnp
from jax import lax
from jax.experimental import pallas as pl
from jax.experimental.pallas import tpu as pltpu
from jax.sharding import PartitionSpec as P

INFLATION = 1.2
NS_STEPS = 16
NS_UNROLL = 3
FULL = lax.Precision.HIGHEST
MESH = pl.DeviceIdType.MESH
BF16 = jnp.bfloat16
F32 = jnp.float32
LANES = 128
PREV_LANE = 72
NEXT_LANE = 96
GAIN_LANE = 127


def split3(x):
    hi = x.astype(BF16)
    rest = x - hi.astype(F32)
    mid = rest.astype(BF16)
    lo = (rest - mid.astype(F32)).astype(BF16)
    return hi, mid, lo


def lhs_pack(x):
    hi, mid, lo = split3(x)
    return jnp.concatenate([hi, mid, hi, mid, hi, lo], axis=1)


def rhs_pack(x):
    hi, mid, lo = split3(x)
    return jnp.concatenate([hi, hi, mid, mid, lo, hi], axis=0)


def dot32(lhs, rhs):
    return jnp.dot(lhs, rhs, preferred_element_type=F32)


def kernel(num_dev, num_cycles, num_obs, halo,
           obs_ref, x_ref, a_ref, win_ref, wout_ref, y_ref, r_ref,
           out_ref,
           state, win_s, wout_s, send1, land1, send2, land2, xz, yprev, ynext, yall,
           s1, r1, s2, r2, sy0, ry0, sy1, ry1):
    me = lax.axis_index('ens')
    num_cols, num_vars = x_ref.shape
    num_layers = win_ref.shape[0]
    blk = num_cols // num_dev
    num_mem = num_dev

    bar = pltpu.get_barrier_semaphore()
    def greet(i, carry):
        pl.semaphore_signal(bar, inc=1, device_id={'ens': lax.rem(me + i, num_dev)}, device_id_type=MESH)
        return carry
    lax.fori_loop(1, num_dev, greet, 0)

    var = lax.broadcasted_iota(jnp.int32, (LANES, LANES), 0)
    lane = lax.broadcasted_iota(jnp.int32, (LANES, LANES), 1)
    place = var + num_obs
    for i in range(num_obs):
        place = place - jnp.where(var > obs_ref[i], 1, 0)
    for i in range(num_obs):
        place = jnp.where(var == obs_ref[i], i, place)
    to_lane = jnp.where((place == lane) & (var < num_vars), 1.0, 0.0).astype(F32)
    to_lane_b = to_lane.astype(BF16)
    eye = jnp.where(var == lane, 1.0, 0.0).astype(F32)

    state[...] = jnp.dot(x_ref[...], to_lane[:num_vars], precision=FULL, preferred_element_type=F32)
    for l in range(num_layers):
        win_s[l] = lax.dot_general(to_lane_b[:num_vars], win_ref[l], (((0,), (0,)), ((), ())),
                                   preferred_element_type=F32).astype(BF16)
        wout_s[l] = jnp.dot(wout_ref[l], to_lane_b[:num_vars], preferred_element_type=F32).astype(BF16)

    send1_rows = send1.reshape(num_cols, LANES)
    land1_rows = land1.reshape(num_mem * blk, LANES)
    send2_rows = send2.reshape(num_mem * blk, LANES)
    land2_rows = land2.reshape(num_cols, LANES)

    def scatter(src, dst, ss, rs):
        def body(i, carry):
            peer = lax.rem(me + i, num_dev)
            pltpu.make_async_remote_copy(src_ref=src.at[peer], dst_ref=dst.at[me], send_sem=ss, recv_sem=rs,
                                         device_id={'ens': peer}, device_id_type=MESH).start()
            return carry
        lax.fori_loop(1, num_dev, body, 0)
        dst[pl.ds(me, 1)] = src[pl.ds(me, 1)]

    def settle(src, dst, ss, rs):
        pltpu.make_async_copy(src.at[pl.ds(0, num_dev - 1)], dst.at[pl.ds(0, num_dev - 1)], ss).wait()
        pltpu.make_async_copy(src.at[pl.ds(0, num_dev - 1)], dst.at[pl.ds(0, num_dev - 1)], rs).wait()

    def y_copies():
        right = lax.rem(me + 1, num_dev)
        left = lax.rem(me + num_dev - 1, num_dev)
        return (pltpu.make_async_remote_copy(src_ref=y_ref, dst_ref=yprev, send_sem=sy0, recv_sem=ry0,
                                             device_id={'ens': right}, device_id_type=MESH),
                pltpu.make_async_remote_copy(src_ref=y_ref, dst_ref=ynext, send_sem=sy1, recv_sem=ry1,
                                             device_id={'ens': left}, device_id_type=MESH))

    TILE = 128
    def forecast():
        for l in range(num_layers):
            hb = state[...].astype(BF16)
            for t in range(num_cols // TILE):
                rows = pl.ds(t * TILE, TILE)
                mixed = jnp.dot(a_ref[rows, :], hb, preferred_element_type=F32).astype(BF16)
                hidden = jnp.dot(mixed, win_s[l], preferred_element_type=F32)
                act = jax.nn.gelu(hidden, approximate=True).astype(BF16)
                state[rows, :] += jnp.dot(act, wout_s[l], preferred_element_type=F32)

    lane_row = lax.broadcasted_iota(jnp.int32, (num_cols, LANES), 1)
    col_row = lax.broadcasted_iota(jnp.int32, (num_cols, LANES), 0) % blk

    def pack_state():
        h = state[...]
        before = pltpu.roll(h, blk, 0)
        after = pltpu.roll(h, num_cols - blk, 0)
        res = h
        for n in range(2 * halo):
            if n < halo:
                col, src, lane0 = (n - halo) % blk, before, PREV_LANE + n * num_obs
            else:
                col, src, lane0 = n - halo, after, NEXT_LANE + (n - halo) * num_obs
            moved = pltpu.roll(src, lane0, 1)
            here = (lane_row >= lane0) & (lane_row < lane0 + num_obs)
            res = jnp.where(here, jnp.where(col_row == col, moved, 0.0), res)
        send1_rows[...] = res

    mem_lane = lax.broadcasted_iota(jnp.int32, (num_mem, LANES), 1)

    def analyse(cycle):
        raws = [land1_rows[pl.ds(j, num_mem, stride=blk), :] for j in range(blk)]
        halo_sum = raws[0]
        for j in range(1, blk):
            halo_sum = halo_sum + raws[j]
        own = raws[0]
        for j in range(1, blk):
            own = jnp.where(mem_lane >= j * num_obs, pltpu.roll(raws[j], j * num_obs, 1), own)
        obs_raw = jnp.where(mem_lane < blk * num_obs, own, halo_sum)
        unused = ((mem_lane >= blk * num_obs) & (mem_lane < PREV_LANE)) | (mem_lane >= NEXT_LANE + halo * num_obs)
        obs_raw = jnp.where(unused, 0.0, obs_raw)
        obs_mean = jnp.mean(obs_raw, axis=0, keepdims=True)
        pert = obs_raw - obs_mean
        innov = yall[pl.ds(cycle, 1), :] - obs_mean
        r_all = r_ref[...]
        energy = jnp.sum(pert * pert, axis=0, keepdims=True)
        base = (num_mem - 1) / INFLATION
        trace = num_mem * base + jnp.sum(r_all * energy, axis=1, keepdims=True)
        innov_rows = jnp.where(lax.broadcasted_iota(jnp.int32, (LANES, LANES), 0) == GAIN_LANE, innov, 0.0)
        right = jnp.concatenate([pert, innov_rows], axis=0)
        means = []
        for j in range(blk):
            weighted = pert * r_all[j:j + 1]
            res = lax.dot_general(weighted, right, (((1,), (1,)), ((), ())), precision=FULL, preferred_element_type=F32)
            inv = 1.0 / trace[j:j + 1]
            xz[j, :, :LANES] = (res[:, :LANES] + base * eye) * inv
            mean = jnp.mean(raws[j], axis=0, keepdims=True)
            means.append(mean)
            xz[j, :, LANES:] = jnp.where(mem_lane < num_vars, raws[j] - mean, res[:, LANES:])

        def ns_step(k, carry):
            for _ in range(NS_UNROLL):
                lhs, first = [], []
                for j in range(blk):
                    both = xz[j]
                    lhs.append(lhs_pack(1.5 * eye - 0.5 * both[:, :LANES]))
                    res = dot32(lhs[j], rhs_pack(both))
                    xz[j, :, LANES:] = res[:, LANES:]
                    first.append(res[:, :LANES])
                for j in range(blk):
                    xz[j, :, :LANES] = dot32(lhs[j], rhs_pack(first[j]))
            return carry
        lax.fori_loop(0, (NS_STEPS - 1) // NS_UNROLL, ns_step, 0)

        for j in range(blk):
            factor = 1.5 * eye - 0.5 * xz[j, :, :LANES]
            fin = dot32(lhs_pack(factor), rhs_pack(xz[j, :, LANES:]))
            inv = 1.0 / trace[j:j + 1]
            shift = jnp.sum(fin * fin[:, GAIN_LANE:GAIN_LANE + 1], axis=0, keepdims=True) * inv
            new = means[j] + shift + (math.sqrt(num_mem - 1) * jnp.sqrt(inv)) * fin
            send2_rows[pl.ds(j, num_mem, stride=blk), :] = jnp.where(mem_lane < num_vars, new, 0.0)

    def cycle_body(cycle, carry):
        forecast()
        pack_state()
        @pl.when(cycle == 0)
        def _():
            pl.semaphore_wait(bar, num_dev - 1)
            for copy in y_copies():
                copy.start()
        scatter(send1, land1, s1, r1)
        @pl.when(cycle == 0)
        def _():
            for copy in y_copies():
                copy.wait()
            ylane = lax.broadcasted_iota(jnp.int32, (num_cycles, LANES), 1)
            width = halo * num_obs
            prev = pltpu.roll(yprev[...], PREV_LANE - (blk - halo) * num_obs, 1)
            nxt = pltpu.roll(ynext[...], NEXT_LANE, 1)
            full = y_ref[...]
            full = jnp.where((ylane >= PREV_LANE) & (ylane < PREV_LANE + width), prev, full)
            full = jnp.where((ylane >= NEXT_LANE) & (ylane < NEXT_LANE + width), nxt, full)
            yall[...] = full
        settle(send1, land1, s1, r1)
        analyse(cycle)
        scatter(send2, land2, s2, r2)
        settle(send2, land2, s2, r2)
        state[...] = land2_rows[...]
        return carry
    lax.fori_loop(0, num_cycles, cycle_body, 0)

    final = lax.dot_general(state[...], to_lane, (((1,), (1,)), ((), ())), precision=FULL, preferred_element_type=F32)
    out_ref[...] = final[:, :num_vars]


def solution(mesh):
    num_dev = mesh.shape['ens']

    def local_run(x_blk, a_mix, w_in, w_out, y_blk, r_blk, obs_idx):
        _, num_cols, num_vars = x_blk.shape
        num_cycles, blk, num_obs = y_blk.shape
        halo = (r_blk.shape[1] - 1) // 2
        num_layers, _, num_hid = w_in.shape
        y_flat = jnp.pad(y_blk.reshape(num_cycles, blk * num_obs), ((0, 0), (0, LANES - blk * num_obs)))
        spread = jnp.stack([jnp.pad(r_blk[j], ((j, blk - 1 - j), (0, 0))) for j in range(blk)])
        spread = spread.reshape(blk, (blk + 2 * halo) * num_obs)
        width = halo * num_obs
        prev, own, nxt = spread[:, :width], spread[:, width:width + blk * num_obs], spread[:, width + blk * num_obs:]
        r_all = jnp.concatenate([
            own, jnp.zeros((blk, PREV_LANE - blk * num_obs), F32), prev,
            jnp.zeros((blk, NEXT_LANE - PREV_LANE - width), F32), nxt,
            jnp.zeros((blk, LANES - NEXT_LANE - width), F32)], axis=1)
        vmem = pl.BlockSpec(memory_space=pltpu.VMEM)
        block = pltpu.VMEM((num_dev, blk, LANES), F32)
        out = pl.pallas_call(
            functools.partial(kernel, num_dev, num_cycles, num_obs, halo),
            out_shape=jax.ShapeDtypeStruct((num_cols, num_vars), F32),
            in_specs=[pl.BlockSpec(memory_space=pltpu.SMEM)] + [vmem] * 6,
            out_specs=vmem,
            scratch_shapes=[
                pltpu.VMEM((num_cols, LANES), F32),
                pltpu.VMEM((num_layers, LANES, num_hid), BF16),
                pltpu.VMEM((num_layers, num_hid, LANES), BF16),
                block, block, block, block,
                pltpu.VMEM((blk, num_dev, 2 * LANES), F32),
                pltpu.VMEM((num_cycles, LANES), F32),
                pltpu.VMEM((num_cycles, LANES), F32),
                pltpu.VMEM((num_cycles, LANES), F32),
            ] + [pltpu.SemaphoreType.DMA] * 8,
            compiler_params=pltpu.CompilerParams(collective_id=0, has_side_effects=True),
        )(obs_idx, x_blk[0], a_mix, w_in, w_out, y_flat, r_all)
        return out[None]

    row_spec = P(('case', 'ens'), None, None)
    return jax.shard_map(local_run, mesh=mesh,
                         in_specs=(row_spec, P(), P(), P(), P(None, ('case', 'ens'), None), row_spec, P()),
                         out_specs=row_spec, check_vma=False)
```

```python
import functools
import math
import random
import jax
import jax.numpy as jnp
from jax import lax
from jax.experimental import pallas as pl
from jax.experimental.pallas import tpu as pltpu
from jax.sharding import PartitionSpec as P

INFLATION = 1.2
NS_STEPS = 16
NS_UNROLL = 3
FULL = lax.Precision.HIGHEST
MESH = pl.DeviceIdType.MESH
BF16 = jnp.bfloat16
F32 = jnp.float32
LANES = 128
PREV_LANE = 72
NEXT_LANE = 96
GAIN_LANE = 127
ROWS = 80


def split3(x):
    hi = x.astype(BF16)
    rest = x - hi.astype(F32)
    mid = rest.astype(BF16)
    lo = (rest - mid.astype(F32)).astype(BF16)
    return hi, mid, lo


def lhs_pack(x):
    hi, mid, lo = split3(x)
    return jnp.concatenate([hi, mid, hi, mid, hi, lo], axis=1)


def rhs_pack(x):
    hi, mid, lo = split3(x)
    return jnp.concatenate([hi, hi, mid, mid, lo, hi], axis=0)


def far_first(side):
    offsets = [(z, y, x, c) for z in range(side) for y in range(side) for x in range(side) for c in range(2)][1:]
    random.Random(1).shuffle(offsets)
    return sorted(offsets, key=lambda o: -sum(min(d, side - d) for d in o[:3]))


def gelu(x):
    half = 0.5 * x
    scale = math.sqrt(2 / math.pi)
    return half + half * jnp.tanh(x * (scale + (scale * 0.044715) * (x * x)))


def dot32(lhs, rhs):
    return jnp.dot(lhs, rhs, preferred_element_type=F32)


def kernel(num_dev, num_cycles, num_obs, halo,
           obs_ref, x_ref, a_ref, win_ref, wout_ref, y_ref, r_ref,
           out_ref,
           state, mix_s, win_s, wout_s, send1, land1, send2, land2, xz, yprev, ynext, yall,
           s1, r1, s2, r2, sy0, ry0, sy1, ry1):
    me = lax.axis_index('ens')
    num_vars, num_cols = x_ref.shape
    num_layers = win_ref.shape[0]
    blk = num_cols // num_dev
    num_mem = num_dev

    bar = pltpu.get_barrier_semaphore()
    def greet(i, carry):
        pl.semaphore_signal(bar, inc=1, device_id={'ens': lax.rem(me + i, num_dev)}, device_id_type=MESH)
        return carry
    lax.fori_loop(1, num_dev, greet, 0)

    def order(dim):
        var = lax.broadcasted_iota(jnp.int32, (LANES, LANES), dim)
        slot = lax.broadcasted_iota(jnp.int32, (LANES, LANES), 1 - dim)
        place = var + num_obs
        for i in range(num_obs):
            place = place - jnp.where(var > obs_ref[i], 1, 0)
        for i in range(num_obs):
            place = jnp.where(var == obs_ref[i], i, place)
        return jnp.where((place == slot) & (var < num_vars), 1.0, 0.0).astype(F32)
    var_slot = order(0)[:num_vars]
    slot_var = order(1)[:, :num_vars]
    eye = jnp.where(lax.broadcasted_iota(jnp.int32, (LANES, LANES), 0)
                    == lax.broadcasted_iota(jnp.int32, (LANES, LANES), 1), 1.0, 0.0).astype(F32)
    eye_cols = jnp.where(lax.broadcasted_iota(jnp.int32, (num_cols, num_cols), 0)
                         == lax.broadcasted_iota(jnp.int32, (num_cols, num_cols), 1), 1.0, 0.0).astype(BF16)

    state[...] = jnp.dot(slot_var[:ROWS], x_ref[...], precision=FULL, preferred_element_type=F32)
    mix_s[...] = lax.dot_general(eye_cols, a_ref[...], (((1,), (1,)), ((), ())),
                                 preferred_element_type=F32).astype(BF16)
    for l in range(num_layers):
        win_s[l] = jnp.dot(win_ref[l], var_slot.astype(BF16), preferred_element_type=F32).astype(BF16)
        wout_s[l] = jnp.dot(slot_var[:ROWS].astype(BF16), wout_ref[l], preferred_element_type=F32).astype(BF16)

    send1_rows = send1.reshape(num_cols, LANES)
    land1_rows = land1.reshape(num_mem * blk, LANES)
    send2_rows = send2.reshape(num_mem * blk, LANES)
    land2_rows = land2.reshape(num_cols, LANES)

    side = 4
    chip = me // 2
    z_at = [(chip // (side * side) + d) % side * (2 * side * side) for d in range(side)]
    y_at = [(chip // side % side + d) % side * (2 * side) for d in range(side)]
    x_at = [(chip % side + d) % side * 2 for d in range(side)]
    c_at = [(me + d) % 2 for d in range(2)]

    def scatter(src, dst, ss, rs):
        for dz, dy, dx, dc in far_first(side):
            peer = z_at[dz] + y_at[dy] + x_at[dx] + c_at[dc]
            pltpu.make_async_remote_copy(src_ref=src.at[peer], dst_ref=dst.at[me], send_sem=ss, recv_sem=rs,
                                         device_id={'ens': peer}, device_id_type=MESH).start()
        dst[pl.ds(me, 1)] = src[pl.ds(me, 1)]

    def settle(src, dst, ss, rs):
        pltpu.make_async_copy(src.at[pl.ds(0, num_dev - 1)], dst.at[pl.ds(0, num_dev - 1)], ss).wait()
        pltpu.make_async_copy(src.at[pl.ds(0, num_dev - 1)], dst.at[pl.ds(0, num_dev - 1)], rs).wait()

    def y_copies():
        right = lax.rem(me + 1, num_dev)
        left = lax.rem(me + num_dev - 1, num_dev)
        return (pltpu.make_async_remote_copy(src_ref=y_ref, dst_ref=yprev, send_sem=sy0, recv_sem=ry0,
                                             device_id={'ens': right}, device_id_type=MESH),
                pltpu.make_async_remote_copy(src_ref=y_ref, dst_ref=ynext, send_sem=sy1, recv_sem=ry1,
                                             device_id={'ens': left}, device_id_type=MESH))

    TILE = 128
    def forecast():
        for l in range(num_layers):
            mixed = dot32(state[...].astype(BF16), mix_s[...]).astype(BF16)
            mixed = jnp.concatenate([mixed, jnp.zeros((LANES - ROWS, num_cols), BF16)], axis=0)
            acts = []
            for t in range(win_s.shape[1] // TILE):
                acts.append(gelu(dot32(win_s[l, pl.ds(t * TILE, TILE), :], mixed)).astype(BF16))
            state[...] += dot32(wout_s[l], jnp.concatenate(acts, axis=0))

    own_col = lax.broadcasted_iota(jnp.int32, (num_obs, num_cols), 1) % blk

    def pack_state():
        obs = state[:num_obs, :]
        before = pltpu.roll(obs, blk, 1)
        after = pltpu.roll(obs, num_cols - blk, 1)
        parts = [state[:PREV_LANE, :]]
        for n in range(halo):
            parts.append(jnp.where(own_col == (n - halo) % blk, before, 0.0))
        for n in range(halo):
            parts.append(jnp.where(own_col == n, after, 0.0))
        parts.append(jnp.zeros((LANES - PREV_LANE - 2 * halo * num_obs, num_cols), F32))
        send1_rows[...] = jnp.concatenate(parts, axis=0).T

    mem_lane = lax.broadcasted_iota(jnp.int32, (num_mem, LANES), 1)

    def analyse(cycle):
        raws = [land1_rows[pl.ds(j, num_mem, stride=blk), :] for j in range(blk)]
        halo_sum = raws[0]
        for j in range(1, blk):
            halo_sum = halo_sum + raws[j]
        own = raws[0]
        for j in range(1, blk):
            own = jnp.where(mem_lane >= j * num_obs, pltpu.roll(raws[j], j * num_obs, 1), own)
        obs_raw = jnp.where(mem_lane < blk * num_obs, own, halo_sum)
        unused = ((mem_lane >= blk * num_obs) & (mem_lane < PREV_LANE)) | (mem_lane >= NEXT_LANE + halo * num_obs)
        obs_raw = jnp.where(unused, 0.0, obs_raw)
        obs_mean = jnp.mean(obs_raw, axis=0, keepdims=True)
        pert = obs_raw - obs_mean
        innov = yall[pl.ds(cycle, 1), :] - obs_mean
        r_all = r_ref[...]
        energy = jnp.sum(pert * pert, axis=0, keepdims=True)
        base = (num_mem - 1) / INFLATION
        trace = num_mem * base + jnp.sum(r_all * energy, axis=1, keepdims=True)
        innov_rows = jnp.where(lax.broadcasted_iota(jnp.int32, (LANES, LANES), 0) == GAIN_LANE, innov, 0.0)
        right = jnp.concatenate([pert, innov_rows], axis=0)
        means = []
        for j in range(blk):
            weighted = pert * r_all[j:j + 1]
            res = lax.dot_general(weighted, right, (((1,), (1,)), ((), ())), precision=FULL, preferred_element_type=F32)
            inv = 1.0 / trace[j:j + 1]
            xz[j, :, :LANES] = (res[:, :LANES] + base * eye) * inv
            mean = jnp.mean(raws[j], axis=0, keepdims=True)
            means.append(mean)
            xz[j, :, LANES:] = jnp.where(mem_lane < num_vars, raws[j] - mean, res[:, LANES:])

        def ns_step(k, carry):
            for _ in range(NS_UNROLL):
                lhs, first = [], []
                for j in range(blk):
                    both = xz[j]
                    lhs.append(lhs_pack(1.5 * eye - 0.5 * both[:, :LANES]))
                    res = dot32(lhs[j], rhs_pack(both))
                    xz[j, :, LANES:] = res[:, LANES:]
                    first.append(res[:, :LANES])
                for j in range(blk):
                    xz[j, :, :LANES] = dot32(lhs[j], rhs_pack(first[j]))
            return carry
        lax.fori_loop(0, (NS_STEPS - 1) // NS_UNROLL, ns_step, 0)

        for j in range(blk):
            factor = 1.5 * eye - 0.5 * xz[j, :, :LANES]
            fin = dot32(lhs_pack(factor), rhs_pack(xz[j, :, LANES:]))
            inv = 1.0 / trace[j:j + 1]
            shift = jnp.sum(fin * fin[:, GAIN_LANE:GAIN_LANE + 1], axis=0, keepdims=True) * inv
            new = means[j] + shift + (math.sqrt(num_mem - 1) * jnp.sqrt(inv)) * fin
            send2_rows[pl.ds(j, num_mem, stride=blk), :] = jnp.where(mem_lane < num_vars, new, 0.0)

    def cycle_body(cycle, carry):
        forecast()
        pack_state()
        @pl.when(cycle == 0)
        def _():
            pl.semaphore_wait(bar, num_dev - 1)
            for copy in y_copies():
                copy.start()
        scatter(send1, land1, s1, r1)
        @pl.when(cycle == 0)
        def _():
            for copy in y_copies():
                copy.wait()
            ylane = lax.broadcasted_iota(jnp.int32, (num_cycles, LANES), 1)
            width = halo * num_obs
            prev = pltpu.roll(yprev[...], PREV_LANE - (blk - halo) * num_obs, 1)
            nxt = pltpu.roll(ynext[...], NEXT_LANE, 1)
            full = y_ref[...]
            full = jnp.where((ylane >= PREV_LANE) & (ylane < PREV_LANE + width), prev, full)
            full = jnp.where((ylane >= NEXT_LANE) & (ylane < NEXT_LANE + width), nxt, full)
            yall[...] = full
        settle(send1, land1, s1, r1)
        analyse(cycle)
        scatter(send2, land2, s2, r2)
        settle(send2, land2, s2, r2)
        state[...] = land2_rows[...].T[:ROWS]
        return carry
    lax.fori_loop(0, num_cycles, cycle_body, 0)

    out_ref[...] = jnp.dot(var_slot[:, :ROWS], state[...], precision=FULL, preferred_element_type=F32)


def solution(mesh):
    num_dev = mesh.shape['ens']

    def local_run(x_blk, a_mix, w_in, w_out, y_blk, r_blk, obs_idx):
        _, num_cols, num_vars = x_blk.shape
        num_cycles, blk, num_obs = y_blk.shape
        halo = (r_blk.shape[1] - 1) // 2
        num_layers, _, num_hid = w_in.shape
        y_flat = jnp.pad(y_blk.reshape(num_cycles, blk * num_obs), ((0, 0), (0, LANES - blk * num_obs)))
        spread = jnp.stack([jnp.pad(r_blk[j], ((j, blk - 1 - j), (0, 0))) for j in range(blk)])
        spread = spread.reshape(blk, (blk + 2 * halo) * num_obs)
        width = halo * num_obs
        prev, own, nxt = spread[:, :width], spread[:, width:width + blk * num_obs], spread[:, width + blk * num_obs:]
        r_all = jnp.concatenate([
            own, jnp.zeros((blk, PREV_LANE - blk * num_obs), F32), prev,
            jnp.zeros((blk, NEXT_LANE - PREV_LANE - width), F32), nxt,
            jnp.zeros((blk, LANES - NEXT_LANE - width), F32)], axis=1)
        vmem = pl.BlockSpec(memory_space=pltpu.VMEM)
        block = pltpu.VMEM((num_dev, blk, LANES), F32)
        out = pl.pallas_call(
            functools.partial(kernel, num_dev, num_cycles, num_obs, halo),
            out_shape=jax.ShapeDtypeStruct((num_vars, num_cols), F32),
            in_specs=[pl.BlockSpec(memory_space=pltpu.SMEM)] + [vmem] * 6,
            out_specs=vmem,
            scratch_shapes=[
                pltpu.VMEM((ROWS, num_cols), F32),
                pltpu.VMEM((num_cols, num_cols), BF16),
                pltpu.VMEM((num_layers, num_hid, LANES), BF16),
                pltpu.VMEM((num_layers, ROWS, num_hid), BF16),
                block, block, block, block,
                pltpu.VMEM((blk, num_dev, 2 * LANES), F32),
                pltpu.VMEM((num_cycles, LANES), F32),
                pltpu.VMEM((num_cycles, LANES), F32),
                pltpu.VMEM((num_cycles, LANES), F32),
            ] + [pltpu.SemaphoreType.DMA] * 8,
            compiler_params=pltpu.CompilerParams(collective_id=0, has_side_effects=True),
        )(obs_idx, x_blk[0].T, a_mix, jnp.swapaxes(w_in, 1, 2), jnp.swapaxes(w_out, 1, 2), y_flat, r_all)
        return out.T[None]

    row_spec = P(('case', 'ens'), None, None)
    return jax.shard_map(local_run, mesh=mesh,
                         in_specs=(row_spec, P(), P(), P(), P(None, ('case', 'ens'), None), row_spec, P()),
                         out_specs=row_spec, check_vma=False)
```

```python
import functools
import math
import random
import jax
import jax.numpy as jnp
from jax import lax
from jax.experimental import pallas as pl
from jax.experimental.pallas import tpu as pltpu
from jax.sharding import PartitionSpec as P

INFLATION = 1.2
NS_STEPS = 16
FULL = lax.Precision.HIGHEST
MESH = pl.DeviceIdType.MESH
BF16 = jnp.bfloat16
F32 = jnp.float32
LANES = 128
PREV_LANE = 72
NEXT_LANE = 96
GAIN_LANE = 127
ROWS = 80


def split3(x):
    hi = x.astype(BF16)
    rest = x - hi.astype(F32)
    mid = rest.astype(BF16)
    lo = (rest - mid.astype(F32)).astype(BF16)
    return hi, mid, lo


def lhs_pack(x):
    hi, mid, lo = split3(x)
    return jnp.concatenate([hi, mid, hi, mid, hi, lo], axis=1)


def rhs_pack(x):
    hi, mid, lo = split3(x)
    return jnp.concatenate([hi, hi, mid, mid, lo, hi], axis=0)


def far_first(side):
    offsets = [(z, y, x, c) for z in range(side) for y in range(side) for x in range(side) for c in range(2)][1:]
    random.Random(1).shuffle(offsets)
    return sorted(offsets, key=lambda o: -sum(min(d, side - d) for d in o[:3]))


def gelu_of_double(u):
    scale = math.sqrt(2 / math.pi)
    return u + u * jnp.tanh(u * (2 * scale + (8 * scale * 0.044715) * (u * u)))


def dot32(lhs, rhs):
    return jnp.dot(lhs, rhs, preferred_element_type=F32)


def kernel(num_dev, num_cycles, num_obs, halo,
           obs_ref, x_ref, a_ref, win_ref, wout_ref, y_in, r_in,
           out_ref,
           state, mix_s, win_s, wout_s, send1, land1, send2, land2, y_ref, yprev, ynext, yall, wide, r_ref,
           s1, r1, s2, r2, sy0, ry0, sy1, ry1):
    me = lax.axis_index('ens')
    num_vars, _, num_cols = x_ref.shape
    num_layers = win_ref.shape[0]
    blk = num_cols // num_dev
    num_mem = num_dev

    bar = pltpu.get_barrier_semaphore()
    def greet(i, carry):
        pl.semaphore_signal(bar, inc=1, device_id={'ens': lax.rem(me + i, num_dev)}, device_id_type=MESH)
        return carry
    lax.fori_loop(1, num_dev, greet, 0)

    def order(dim):
        var = lax.broadcasted_iota(jnp.int32, (LANES, LANES), dim)
        slot = lax.broadcasted_iota(jnp.int32, (LANES, LANES), 1 - dim)
        place = var + num_obs
        for i in range(num_obs):
            place = place - jnp.where(var > obs_ref[i], 1, 0)
        for i in range(num_obs):
            place = jnp.where(var == obs_ref[i], i, place)
        return jnp.where((place == slot) & (var < num_vars), 1.0, 0.0).astype(F32)
    var_slot = order(0)[:num_vars]
    slot_var = order(1)[:, :num_vars]
    eye = jnp.where(lax.broadcasted_iota(jnp.int32, (LANES, LANES), 0)
                    == lax.broadcasted_iota(jnp.int32, (LANES, LANES), 1), 1.0, 0.0).astype(F32)
    eye_cols = jnp.where(lax.broadcasted_iota(jnp.int32, (num_cols, num_cols), 0)
                         == lax.broadcasted_iota(jnp.int32, (num_cols, num_cols), 1), 1.0, 0.0).astype(BF16)

    state[...] = jnp.dot(slot_var[:ROWS], x_ref[:, 0, :], precision=FULL, preferred_element_type=F32)
    mix_s[...] = lax.dot_general(eye_cols, a_ref[...], (((1,), (1,)), ((), ())),
                                 preferred_element_type=F32).astype(BF16)
    for l in range(num_layers):
        win_s[l] = (0.5 * jnp.dot(win_ref[l], var_slot.astype(BF16), preferred_element_type=F32)).astype(BF16)
        wout_s[l] = jnp.dot(slot_var[:ROWS].astype(BF16), wout_ref[l], preferred_element_type=F32).astype(BF16)

    send1_rows = send1.reshape(num_cols, LANES)
    land1_rows = land1.reshape(num_mem * blk, LANES)
    send2_rows = send2.reshape(num_mem * blk, LANES)
    land2_rows = land2.reshape(num_cols, LANES)

    side = 4
    chip = me // 2
    z_at = [(chip // (side * side) + d) % side * (2 * side * side) for d in range(side)]
    y_at = [(chip // side % side + d) % side * (2 * side) for d in range(side)]
    x_at = [(chip % side + d) % side * 2 for d in range(side)]
    c_at = [(me + d) % 2 for d in range(2)]

    def scatter(src, dst, ss, rs):
        for dz, dy, dx, dc in far_first(side):
            peer = z_at[dz] + y_at[dy] + x_at[dx] + c_at[dc]
            pltpu.make_async_remote_copy(src_ref=src.at[peer], dst_ref=dst.at[me], send_sem=ss, recv_sem=rs,
                                         device_id={'ens': peer}, device_id_type=MESH).start()
        dst[pl.ds(me, 1)] = src[pl.ds(me, 1)]

    def settle(src, dst, ss, rs):
        pltpu.make_async_copy(src.at[pl.ds(0, num_dev - 1)], dst.at[pl.ds(0, num_dev - 1)], ss).wait()
        pltpu.make_async_copy(src.at[pl.ds(0, num_dev - 1)], dst.at[pl.ds(0, num_dev - 1)], rs).wait()

    def place_lanes():
        wide[...] = jnp.zeros_like(wide)
        for j in range(blk):
            wide[j, :num_cycles, :num_obs] = y_in[:, j, :]
        for o in range(2 * halo + 1):
            wide[blk + o, :blk, :num_obs] = r_in[o]
        full = wide[0]
        for j in range(1, blk):
            full = full + pltpu.roll(wide[j], j * num_obs, 1)
        y_ref[...] = full[:num_cycles]
        row = lax.broadcasted_iota(jnp.int32, (8, LANES), 0)
        full = jnp.zeros((8, LANES), F32)
        for j in range(blk):
            for o in range(2 * halo + 1):
                col = j + o - halo
                if col < 0:
                    at = PREV_LANE + (col + halo) * num_obs
                elif col < blk:
                    at = col * num_obs
                else:
                    at = NEXT_LANE + (col - blk) * num_obs
                moved = wide[blk + o] if at == 0 else pltpu.roll(wide[blk + o], at, 1)
                full = full + jnp.where(row == j, moved, 0.0)
        r_ref[...] = full
    place_lanes()

    def y_copies():
        right = lax.rem(me + 1, num_dev)
        left = lax.rem(me + num_dev - 1, num_dev)
        return (pltpu.make_async_remote_copy(src_ref=y_ref, dst_ref=yprev, send_sem=sy0, recv_sem=ry0,
                                             device_id={'ens': right}, device_id_type=MESH),
                pltpu.make_async_remote_copy(src_ref=y_ref, dst_ref=ynext, send_sem=sy1, recv_sem=ry1,
                                             device_id={'ens': left}, device_id_type=MESH))

    TILE = 256
    def forecast():
        for l in range(num_layers):
            mixed = dot32(state[...].astype(BF16), mix_s[...]).astype(BF16)
            mixed = jnp.concatenate([mixed, jnp.zeros((LANES - ROWS, num_cols), BF16)], axis=0)
            acts = []
            for c in range(num_cols // TILE):
                hidden = []
                for t in range(win_s.shape[1] // TILE):
                    half = dot32(win_s[l, pl.ds(t * TILE, TILE), :], mixed[:, c * TILE:(c + 1) * TILE])
                    hidden.append(gelu_of_double(half).astype(BF16))
                acts.append(jnp.concatenate(hidden, axis=0))
            for c in range(num_cols // TILE):
                state[:, c * TILE:(c + 1) * TILE] += dot32(wout_s[l], acts[c])

    own_col = lax.broadcasted_iota(jnp.int32, (num_obs, num_cols), 1) % blk

    def pack_state():
        obs = state[:num_obs, :]
        before = pltpu.roll(obs, blk, 1)
        after = pltpu.roll(obs, num_cols - blk, 1)
        parts = [state[:PREV_LANE, :]]
        for n in range(halo):
            parts.append(jnp.where(own_col == (n - halo) % blk, before, 0.0))
        for n in range(halo):
            parts.append(jnp.where(own_col == n, after, 0.0))
        parts.append(jnp.zeros((LANES - PREV_LANE - 2 * halo * num_obs, num_cols), F32))
        send1_rows[...] = jnp.concatenate(parts, axis=0).T

    mem_lane = lax.broadcasted_iota(jnp.int32, (num_mem, LANES), 1)

    def analyse(cycle):
        raws = [land1_rows[pl.ds(j, num_mem, stride=blk), :] for j in range(blk)]
        halo_sum = raws[0]
        for j in range(1, blk):
            halo_sum = halo_sum + raws[j]
        own = raws[0]
        for j in range(1, blk):
            own = jnp.where(mem_lane >= j * num_obs, pltpu.roll(raws[j], j * num_obs, 1), own)
        obs_raw = jnp.where(mem_lane < blk * num_obs, own, halo_sum)
        unused = ((mem_lane >= blk * num_obs) & (mem_lane < PREV_LANE)) | (mem_lane >= NEXT_LANE + halo * num_obs)
        obs_raw = jnp.where(unused, 0.0, obs_raw)
        obs_mean = jnp.mean(obs_raw, axis=0, keepdims=True)
        pert = obs_raw - obs_mean
        innov = yall[pl.ds(cycle, 1), :] - obs_mean
        r_all = r_ref[:blk, :]
        energy = jnp.sum(pert * pert, axis=0, keepdims=True)
        base = (num_mem - 1) / INFLATION
        trace = num_mem * base + jnp.sum(r_all * energy, axis=1, keepdims=True)
        innov_rows = jnp.where(lax.broadcasted_iota(jnp.int32, (LANES, LANES), 0) == GAIN_LANE, innov, 0.0)
        right = jnp.concatenate([pert, innov_rows], axis=0)
        means, xs, zs = [], [], []
        threehalf = 1.5 * eye
        for j in range(blk):
            weighted = pert * r_all[j:j + 1]
            res = lax.dot_general(weighted, right, (((1,), (1,)), ((), ())), precision=FULL, preferred_element_type=F32)
            inv = 1.0 / trace[j:j + 1]
            xs.append((res[:, :LANES] + base * eye) * (0.5 * inv))
            mean = jnp.mean(raws[j], axis=0, keepdims=True)
            means.append(mean)
            zs.append(jnp.where(mem_lane < num_vars, raws[j] - mean, res[:, LANES:]))

        for _ in range(NS_STEPS - 1):
            lhs, first = [], []
            for j in range(blk):
                lhs.append(lhs_pack(threehalf - xs[j]))
                res = dot32(lhs[j], rhs_pack(jnp.concatenate([xs[j], zs[j]], axis=1)))
                first.append(res[:, :LANES])
                zs[j] = res[:, LANES:]
            for j in range(blk):
                hi, mid, lo = split3(first[j])
                pair = jnp.concatenate([hi, mid], axis=1)
                wide = dot32(lhs[j][:, :2 * LANES], jnp.concatenate([pair, pair], axis=0))
                thin = dot32(lhs[j][:, 4 * LANES:], jnp.concatenate([lo, hi], axis=0))
                xs[j] = wide[:, :LANES] + (wide[:, LANES:] + thin)

        for j in range(blk):
            factor = threehalf - xs[j]
            fin = dot32(lhs_pack(factor), rhs_pack(zs[j]))
            inv = 1.0 / trace[j:j + 1]
            shift = jnp.sum(fin * fin[:, GAIN_LANE:GAIN_LANE + 1], axis=0, keepdims=True) * inv
            new = means[j] + shift + (math.sqrt(num_mem - 1) * jnp.sqrt(inv)) * fin
            send2_rows[pl.ds(j, num_mem, stride=blk), :] = jnp.where(mem_lane < num_vars, new, 0.0)

    def cycle_body(cycle, carry):
        forecast()
        @pl.when(cycle == 0)
        def _():
            pl.semaphore_wait(bar, num_dev - 1)
            for copy in y_copies():
                copy.start()
        pack_state()
        scatter(send1, land1, s1, r1)
        @pl.when(cycle == 0)
        def _():
            for copy in y_copies():
                copy.wait()
            ylane = lax.broadcasted_iota(jnp.int32, (num_cycles, LANES), 1)
            width = halo * num_obs
            prev = pltpu.roll(yprev[...], PREV_LANE - (blk - halo) * num_obs, 1)
            nxt = pltpu.roll(ynext[...], NEXT_LANE, 1)
            full = y_ref[...]
            full = jnp.where((ylane >= PREV_LANE) & (ylane < PREV_LANE + width), prev, full)
            full = jnp.where((ylane >= NEXT_LANE) & (ylane < NEXT_LANE + width), nxt, full)
            yall[...] = full
        settle(send1, land1, s1, r1)
        analyse(cycle)
        scatter(send2, land2, s2, r2)
        settle(send2, land2, s2, r2)
        state[...] = land2_rows[...].T[:ROWS]
        return carry
    lax.fori_loop(0, num_cycles, cycle_body, 0)

    out_ref[:, 0, :] = jnp.dot(var_slot[:, :ROWS], state[...], precision=FULL, preferred_element_type=F32)


def solution(mesh):
    num_dev = mesh.shape['ens']

    def local_run(x_blk, a_mix, w_in, w_out, y_blk, r_blk, obs_idx):
        _, num_cols, num_vars = x_blk.shape
        num_cycles, blk, num_obs = y_blk.shape
        halo = (r_blk.shape[1] - 1) // 2
        num_layers, _, num_hid = w_in.shape
        vmem = pl.BlockSpec(memory_space=pltpu.VMEM)
        block = pltpu.VMEM((num_dev, blk, LANES), F32)
        out = pl.pallas_call(
            functools.partial(kernel, num_dev, num_cycles, num_obs, halo),
            out_shape=jax.ShapeDtypeStruct((num_vars, 1, num_cols), F32),
            in_specs=[pl.BlockSpec(memory_space=pltpu.SMEM)] + [vmem] * 6,
            out_specs=vmem,
            scratch_shapes=[
                pltpu.VMEM((ROWS, num_cols), F32),
                pltpu.VMEM((num_cols, num_cols), BF16),
                pltpu.VMEM((num_layers, num_hid, LANES), BF16),
                pltpu.VMEM((num_layers, ROWS, num_hid), BF16),
                block, block, block, block,
                pltpu.VMEM((num_cycles, LANES), F32),
                pltpu.VMEM((num_cycles, LANES), F32),
                pltpu.VMEM((num_cycles, LANES), F32),
                pltpu.VMEM((num_cycles, LANES), F32),
                pltpu.VMEM((blk + 2 * halo + 1, 8, LANES), F32),
                pltpu.VMEM((8, LANES), F32),
            ] + [pltpu.SemaphoreType.DMA] * 8,
            compiler_params=pltpu.CompilerParams(collective_id=0, has_side_effects=True),
        )(obs_idx, jnp.transpose(x_blk, (2, 0, 1)), a_mix, jnp.swapaxes(w_in, 1, 2), jnp.swapaxes(w_out, 1, 2), y_blk, jnp.swapaxes(r_blk, 0, 1))
        return jnp.transpose(out, (1, 2, 0))

    row_spec = P(('case', 'ens'), None, None)
    return jax.shard_map(local_run, mesh=mesh,
                         in_specs=(row_spec, P(), P(), P(), P(None, ('case', 'ens'), None), row_spec, P()),
                         out_specs=row_spec, check_vma=False)
```

```python
import functools
import math
import random
import jax
import jax.numpy as jnp
from jax import lax
from jax.experimental import pallas as pl
from jax.experimental.pallas import tpu as pltpu
from jax.sharding import PartitionSpec as P

INFLATION = 1.2
NS_STEPS = 16
FULL = lax.Precision.HIGHEST
MESH = pl.DeviceIdType.MESH
BF16 = jnp.bfloat16
F32 = jnp.float32
LANES = 128
PART = 24
PART_LANE = 3 * PART
HALO_LANE = 4 * PART
GAIN_LANE = 127
ROWS = 80


def split3(x):
    hi = x.astype(BF16)
    rest = x - hi.astype(F32)
    mid = rest.astype(BF16)
    lo = (rest - mid.astype(F32)).astype(BF16)
    return hi, mid, lo


def lhs_pack(x):
    hi, mid, lo = split3(x)
    return jnp.concatenate([hi, mid, hi, mid, hi, lo], axis=1)


def rhs_pack(x):
    hi, mid, lo = split3(x)
    return jnp.concatenate([hi, hi, mid, mid, lo, hi], axis=0)


def window_lane(col, blk, num_obs):
    if col < 0:
        return (blk + 2 * (col + blk - 1)) * num_obs
    if col < blk:
        return col * num_obs
    return (blk + 2 * (col - blk) + 1) * num_obs


def far_first(side):
    offsets = [(z, y, x, c) for z in range(side) for y in range(side) for x in range(side) for c in range(2)][1:]
    random.Random(1).shuffle(offsets)
    return sorted(offsets, key=lambda o: -sum(min(d, side - d) for d in o[:3]))


def gelu_of_double(u):
    scale = math.sqrt(2 / math.pi)
    return u + u * jnp.tanh(u * (2 * scale + (8 * scale * 0.044715) * (u * u)))


def dot32(lhs, rhs):
    return jnp.dot(lhs, rhs, preferred_element_type=F32)


def kernel(num_dev, num_cycles, num_obs, halo,
           obs_ref, x_ref, a_ref, win_ref, wout_ref, y_in, r_in,
           out_ref,
           state, mix_s, win_s, wout_s, send1, land1, send2, land2, y_ref, yprev, ynext, yall, wide, r_ref,
           s1, r1, s2, r2, sy0, ry0, sy1, ry1):
    me = lax.axis_index('ens')
    num_vars, _, num_cols = x_ref.shape
    num_layers = win_ref.shape[0]
    blk = num_cols // num_dev
    num_mem = num_dev
    rows = blk - 1
    land2[:, rows:, :] = jnp.zeros((num_cols // blk, 1, LANES), F32)

    bar = pltpu.get_barrier_semaphore()
    def greet(i, carry):
        pl.semaphore_signal(bar, inc=1, device_id={'ens': lax.rem(me + i, num_dev)}, device_id_type=MESH)
        return carry
    lax.fori_loop(1, num_dev, greet, 0)

    def order(dim):
        var = lax.broadcasted_iota(jnp.int32, (LANES, LANES), dim)
        slot = lax.broadcasted_iota(jnp.int32, (LANES, LANES), 1 - dim)
        place = var + num_obs
        for i in range(num_obs):
            place = place - jnp.where(var > obs_ref[i], 1, 0)
        for i in range(num_obs):
            place = jnp.where(var == obs_ref[i], i, place)
        return jnp.where((place == slot) & (var < num_vars), 1.0, 0.0).astype(F32)
    var_slot = order(0)[:num_vars]
    slot_var = order(1)[:, :num_vars]
    eye = jnp.where(lax.broadcasted_iota(jnp.int32, (LANES, LANES), 0)
                    == lax.broadcasted_iota(jnp.int32, (LANES, LANES), 1), 1.0, 0.0).astype(F32)
    eye_cols = jnp.where(lax.broadcasted_iota(jnp.int32, (num_cols, num_cols), 0)
                         == lax.broadcasted_iota(jnp.int32, (num_cols, num_cols), 1), 1.0, 0.0).astype(BF16)

    state[...] = jnp.dot(slot_var[:ROWS], x_ref[:, 0, :], precision=FULL, preferred_element_type=F32)
    mix_s[...] = lax.dot_general(eye_cols, a_ref[...], (((1,), (1,)), ((), ())),
                                 preferred_element_type=F32).astype(BF16)
    for l in range(num_layers):
        win_s[l] = (0.5 * jnp.dot(win_ref[l], var_slot.astype(BF16), preferred_element_type=F32)).astype(BF16)
        wout_s[l] = jnp.dot(slot_var[:ROWS].astype(BF16), wout_ref[l], preferred_element_type=F32).astype(BF16)

    send1_rows = send1.reshape(num_cols, LANES)
    land1_rows = land1.reshape(num_mem * blk, LANES)
    send2_rows = send2.reshape(num_mem * blk, LANES)
    land2_rows = land2.reshape(num_cols, LANES)

    side = 4
    chip = me // 2
    z_at = [(chip // (side * side) + d) % side * (2 * side * side) for d in range(side)]
    y_at = [(chip // side % side + d) % side * (2 * side) for d in range(side)]
    x_at = [(chip % side + d) % side * 2 for d in range(side)]
    c_at = [(me + d) % 2 for d in range(2)]

    def scatter(src, dst, ss, rs):
        for dz, dy, dx, dc in far_first(side):
            peer = z_at[dz] + y_at[dy] + x_at[dx] + c_at[dc]
            pltpu.make_async_remote_copy(src_ref=src.at[peer, pl.ds(0, rows)], dst_ref=dst.at[me, pl.ds(0, rows)], send_sem=ss, recv_sem=rs,
                                         device_id={'ens': peer}, device_id_type=MESH).start()
        dst[pl.ds(me, 1), :rows] = src[pl.ds(me, 1), :rows]

    def settle(src, dst, ss, rs):
        sent = src.at[pl.ds(0, num_dev - 1), pl.ds(0, rows)]
        landed = dst.at[pl.ds(0, num_dev - 1), pl.ds(0, rows)]
        pltpu.make_async_copy(sent, landed, ss).wait()
        pltpu.make_async_copy(sent, landed, rs).wait()

    def place_lanes():
        wide[...] = jnp.zeros_like(wide)
        for j in range(blk):
            wide[j, :num_cycles, :num_obs] = y_in[:, j, :]
        for o in range(2 * halo + 1):
            wide[blk + o, :blk, :num_obs] = r_in[o]
        full = wide[0]
        for j in range(1, blk):
            full = full + pltpu.roll(wide[j], j * num_obs, 1)
        y_ref[...] = full[:num_cycles]
        row = lax.broadcasted_iota(jnp.int32, (8, LANES), 0)
        full = jnp.zeros((8, LANES), F32)
        for j in range(blk):
            for o in range(2 * halo + 1):
                at = window_lane(j + o - halo, blk, num_obs)
                moved = wide[blk + o] if at == 0 else pltpu.roll(wide[blk + o], at, 1)
                full = full + jnp.where(row == j, moved, 0.0)
        r_ref[...] = full
    place_lanes()

    def y_copies():
        right = lax.rem(me + 1, num_dev)
        left = lax.rem(me + num_dev - 1, num_dev)
        return (pltpu.make_async_remote_copy(src_ref=y_ref, dst_ref=yprev, send_sem=sy0, recv_sem=ry0,
                                             device_id={'ens': right}, device_id_type=MESH),
                pltpu.make_async_remote_copy(src_ref=y_ref, dst_ref=ynext, send_sem=sy1, recv_sem=ry1,
                                             device_id={'ens': left}, device_id_type=MESH))

    TILE = 256
    def forecast():
        for l in range(num_layers):
            mixed = dot32(state[...].astype(BF16), mix_s[...]).astype(BF16)
            mixed = jnp.concatenate([mixed, jnp.zeros((LANES - ROWS, num_cols), BF16)], axis=0)
            acts = []
            for c in range(num_cols // TILE):
                hidden = []
                for t in range(win_s.shape[1] // TILE):
                    half = dot32(win_s[l, pl.ds(t * TILE, TILE), :], mixed[:, c * TILE:(c + 1) * TILE])
                    hidden.append(gelu_of_double(half).astype(BF16))
                acts.append(jnp.concatenate(hidden, axis=0))
            for c in range(num_cols // TILE):
                state[:, c * TILE:(c + 1) * TILE] += dot32(wout_s[l], acts[c])

    own_col = lax.broadcasted_iota(jnp.int32, (PART, num_cols), 1) % blk

    def pack_state():
        obs = state[:num_obs, :]
        spread = jnp.zeros((PART, num_cols), F32)
        for j in range(rows):
            part = state[j * PART:(j + 1) * PART, :]
            spread = jnp.where(own_col == j, pltpu.roll(part, num_cols - (rows - j), 1), spread)
        send1_rows[...] = jnp.concatenate([
            state[:PART_LANE, :], spread, pltpu.roll(obs, rows, 1), pltpu.roll(obs, num_cols - blk, 1),
            jnp.zeros((LANES - HALO_LANE - 2 * num_obs, num_cols), F32)], axis=0).T

    def unpack_state():
        landed = land2_rows[...].T
        spread = landed[PART_LANE:HALO_LANE]
        for j in range(rows):
            part = landed[j * PART:(j + 1) * PART]
            state[j * PART:(j + 1) * PART, :] = jnp.where(own_col == rows, pltpu.roll(spread, rows - j, 1), part)

    mem_lane = lax.broadcasted_iota(jnp.int32, (num_mem, LANES), 1)

    def analyse(cycle):
        raws = [land1_rows[pl.ds(j, num_mem, stride=blk), :] for j in range(rows)]
        def moved(j, by):
            return pltpu.roll(raws[j], by % LANES, 1)
        second = moved(1, PART - PART_LANE)
        last = jnp.where(mem_lane < PART, moved(0, -PART_LANE), second)
        last = jnp.where(mem_lane < 2 * PART, last, moved(2, 2 * PART - PART_LANE))
        first_halo = blk * num_obs
        pieces = [raws[0], moved(1, num_obs), moved(2, 2 * num_obs), moved(0, 3 * num_obs - PART_LANE),
                  moved(0, first_halo - HALO_LANE), second, moved(2, first_halo + 4 * num_obs - HALO_LANE)]
        ends = [num_obs, 2 * num_obs, 3 * num_obs, 4 * num_obs, 6 * num_obs, 8 * num_obs, 10 * num_obs]
        obs_raw = jnp.zeros((num_mem, LANES), F32)
        for piece, end in reversed(list(zip(pieces, ends))):
            obs_raw = jnp.where(mem_lane < end, piece, obs_raw)
        raws.append(last)
        obs_mean = jnp.mean(obs_raw, axis=0, keepdims=True)
        pert = obs_raw - obs_mean
        innov = yall[pl.ds(cycle, 1), :] - obs_mean
        r_all = r_ref[:blk, :]
        energy = jnp.sum(pert * pert, axis=0, keepdims=True)
        base = (num_mem - 1) / INFLATION
        trace = num_mem * base + jnp.sum(r_all * energy, axis=1, keepdims=True)
        innov_rows = jnp.where(lax.broadcasted_iota(jnp.int32, (LANES, LANES), 0) == GAIN_LANE, innov, 0.0)
        right = jnp.concatenate([pert, innov_rows], axis=0)
        means, xs, zs, news = [], [], [], []
        threehalf = 1.5 * eye
        weighted = jnp.concatenate([pert * r_all[j:j + 1] for j in range(blk)], axis=0)
        gram = dot32(lhs_pack(weighted), rhs_pack(right.T))
        for j in range(blk):
            res = gram[j * num_mem:(j + 1) * num_mem]
            inv = 1.0 / trace[j:j + 1]
            xs.append((res[:, :LANES] + base * eye) * (0.5 * inv))
            mean = jnp.mean(raws[j], axis=0, keepdims=True)
            means.append(mean)
            zs.append(jnp.where(mem_lane < num_vars, raws[j] - mean, res[:, LANES:]))

        for _ in range(NS_STEPS - 1):
            lhs, first = [], []
            for j in range(blk):
                lhs.append(lhs_pack(threehalf - xs[j]))
                res = dot32(lhs[j], rhs_pack(jnp.concatenate([xs[j], zs[j]], axis=1)))
                first.append(res[:, :LANES])
                zs[j] = res[:, LANES:]
            for j in range(blk):
                hi, mid, lo = split3(first[j])
                pair = jnp.concatenate([hi, mid], axis=1)
                wide = dot32(lhs[j][:, :2 * LANES], jnp.concatenate([pair, pair], axis=0))
                thin = dot32(lhs[j][:, 4 * LANES:], jnp.concatenate([lo, hi], axis=0))
                xs[j] = wide[:, :LANES] + (wide[:, LANES:] + thin)

        for j in range(blk):
            factor = threehalf - xs[j]
            fin = dot32(lhs_pack(factor), rhs_pack(zs[j]))
            inv = 1.0 / trace[j:j + 1]
            shift = jnp.sum(fin * fin[:, GAIN_LANE:GAIN_LANE + 1], axis=0, keepdims=True) * inv
            new = means[j] + shift + (math.sqrt(num_mem - 1) * jnp.sqrt(inv)) * fin
            news.append(jnp.where(mem_lane < num_vars, new, 0.0))
        for j in range(rows):
            part = pltpu.roll(news[rows], PART_LANE - j * PART, 1)
            send2_rows[pl.ds(j, num_mem, stride=blk), :] = jnp.where(mem_lane < PART_LANE, news[j], part)

    def cycle_body(cycle, carry):
        forecast()
        @pl.when(cycle == 0)
        def _():
            pl.semaphore_wait(bar, num_dev - 1)
            for copy in y_copies():
                copy.start()
        pack_state()
        scatter(send1, land1, s1, r1)
        @pl.when(cycle == 0)
        def _():
            for copy in y_copies():
                copy.wait()
            ylane = lax.broadcasted_iota(jnp.int32, (num_cycles, LANES), 1)
            full = y_ref[...]
            for n in range(halo):
                for col, src, at in ((n - halo, yprev, blk - halo + n), (blk + n, ynext, n)):
                    to = window_lane(col, blk, num_obs)
                    here = (ylane >= to) & (ylane < to + num_obs)
                    full = jnp.where(here, pltpu.roll(src[...], (to - at * num_obs) % LANES, 1), full)
            yall[...] = full
        settle(send1, land1, s1, r1)
        analyse(cycle)
        scatter(send2, land2, s2, r2)
        settle(send2, land2, s2, r2)
        unpack_state()
        return carry
    lax.fori_loop(0, num_cycles, cycle_body, 0)

    out_ref[:, 0, :] = jnp.dot(var_slot[:, :ROWS], state[...], precision=FULL, preferred_element_type=F32)


def solution(mesh):
    num_dev = mesh.shape['ens']

    def local_run(x_blk, a_mix, w_in, w_out, y_blk, r_blk, obs_idx):
        _, num_cols, num_vars = x_blk.shape
        num_cycles, blk, num_obs = y_blk.shape
        halo = (r_blk.shape[1] - 1) // 2
        num_layers, _, num_hid = w_in.shape
        vmem = pl.BlockSpec(memory_space=pltpu.VMEM)
        block = pltpu.VMEM((num_dev, blk, LANES), F32)
        out = pl.pallas_call(
            functools.partial(kernel, num_dev, num_cycles, num_obs, halo),
            out_shape=jax.ShapeDtypeStruct((num_vars, 1, num_cols), F32),
            in_specs=[pl.BlockSpec(memory_space=pltpu.SMEM)] + [vmem] * 6,
            out_specs=vmem,
            scratch_shapes=[
                pltpu.VMEM((ROWS, num_cols), F32),
                pltpu.VMEM((num_cols, num_cols), BF16),
                pltpu.VMEM((num_layers, num_hid, LANES), BF16),
                pltpu.VMEM((num_layers, ROWS, num_hid), BF16),
                block, block, block, block,
                pltpu.VMEM((num_cycles, LANES), F32),
                pltpu.VMEM((num_cycles, LANES), F32),
                pltpu.VMEM((num_cycles, LANES), F32),
                pltpu.VMEM((num_cycles, LANES), F32),
                pltpu.VMEM((blk + 2 * halo + 1, 8, LANES), F32),
                pltpu.VMEM((8, LANES), F32),
            ] + [pltpu.SemaphoreType.DMA] * 8,
            compiler_params=pltpu.CompilerParams(collective_id=0, has_side_effects=True),
        )(obs_idx, jnp.transpose(x_blk, (2, 0, 1)), a_mix, jnp.swapaxes(w_in, 1, 2), jnp.swapaxes(w_out, 1, 2), y_blk, jnp.swapaxes(r_blk, 0, 1))
        return jnp.transpose(out, (1, 2, 0))

    row_spec = P(('case', 'ens'), None, None)
    return jax.shard_map(local_run, mesh=mesh,
                         in_specs=(row_spec, P(), P(), P(), P(None, ('case', 'ens'), None), row_spec, P()),
                         out_specs=row_spec, check_vma=False)
```

```python
import functools
import math
import random
import jax
import jax.numpy as jnp
from jax import lax
from jax.experimental import pallas as pl
from jax.experimental.pallas import tpu as pltpu
from jax.sharding import PartitionSpec as P

INFLATION = 1.2
NS_STEPS = 16
FULL = lax.Precision.HIGHEST
MESH = pl.DeviceIdType.MESH
BF16 = jnp.bfloat16
F32 = jnp.float32
LANES = 128
PART = 24
PART_LANE = 3 * PART
HALO_LANE = 4 * PART
GAIN_LANE = 127
ROWS = 80


def split3(x):
    hi = x.astype(BF16)
    rest = x - hi.astype(F32)
    mid = rest.astype(BF16)
    lo = (rest - mid.astype(F32)).astype(BF16)
    return hi, mid, lo


def lhs_pack(x):
    hi, mid, lo = split3(x)
    return jnp.concatenate([hi, mid, hi, mid, hi, lo], axis=1)


def rhs_pack(x):
    hi, mid, lo = split3(x)
    return jnp.concatenate([hi, hi, mid, mid, lo, hi], axis=0)


def window_lane(col, blk, num_obs):
    if col < 0:
        return (blk + 2 * (col + blk - 1)) * num_obs
    if col < blk:
        return col * num_obs
    return (blk + 2 * (col - blk) + 1) * num_obs


def far_first(side):
    offsets = [(z, y, x, c) for z in range(side) for y in range(side) for x in range(side) for c in range(2)][1:]
    random.Random(1).shuffle(offsets)
    return sorted(offsets, key=lambda o: -sum(min(d, side - d) for d in o[:3]))


def gelu_of_double(u):
    scale = math.sqrt(2 / math.pi)
    return u + u * jnp.tanh(u * (2 * scale + (8 * scale * 0.044715) * (u * u)))


def dot32(lhs, rhs):
    return jnp.dot(lhs, rhs, preferred_element_type=F32)


def kernel(num_dev, num_cycles, num_obs, halo,
           obs_ref, x_ref, a_ref, win_ref, wout_ref, y_in, r_in,
           out_ref,
           state, mix_s, win_s, wout_s, send1, land1, send2, land2, y_ref, yprev, ynext, yall, wide, r_ref,
           s1, r1, s2, r2, sy0, ry0, sy1, ry1):
    me = lax.axis_index('ens')
    num_vars, _, num_cols = x_ref.shape
    num_layers = win_ref.shape[0]
    blk = num_cols // num_dev
    num_mem = num_dev
    rows = blk - 1
    land2[:, rows:, :] = jnp.zeros((num_cols // blk, 1, LANES), F32)

    bar = pltpu.get_barrier_semaphore()
    def greet(i, carry):
        pl.semaphore_signal(bar, inc=1, device_id={'ens': lax.rem(me + i, num_dev)}, device_id_type=MESH)
        return carry
    lax.fori_loop(1, num_dev, greet, 0)

    def order(dim):
        var = lax.broadcasted_iota(jnp.int32, (LANES, LANES), dim)
        slot = lax.broadcasted_iota(jnp.int32, (LANES, LANES), 1 - dim)
        place = var + num_obs
        for i in range(num_obs):
            place = place - jnp.where(var > obs_ref[i], 1, 0)
        for i in range(num_obs):
            place = jnp.where(var == obs_ref[i], i, place)
        return jnp.where((place == slot) & (var < num_vars), 1.0, 0.0).astype(F32)
    var_slot = order(0)[:num_vars]
    slot_var = order(1)[:, :num_vars]
    eye = jnp.where(lax.broadcasted_iota(jnp.int32, (LANES, LANES), 0)
                    == lax.broadcasted_iota(jnp.int32, (LANES, LANES), 1), 1.0, 0.0).astype(F32)
    eye_cols = jnp.where(lax.broadcasted_iota(jnp.int32, (num_cols, num_cols), 0)
                         == lax.broadcasted_iota(jnp.int32, (num_cols, num_cols), 1), 1.0, 0.0).astype(BF16)

    state[...] = jnp.dot(slot_var[:ROWS], x_ref[:, 0, :], precision=FULL, preferred_element_type=F32)
    mix_s[...] = lax.dot_general(eye_cols, a_ref[...], (((1,), (1,)), ((), ())),
                                 preferred_element_type=F32).astype(BF16)
    for l in range(num_layers):
        win_s[l] = (0.5 * jnp.dot(win_ref[l], var_slot.astype(BF16), preferred_element_type=F32)).astype(BF16)
        wout_s[l] = jnp.dot(slot_var[:ROWS].astype(BF16), wout_ref[l], preferred_element_type=F32).astype(BF16)

    send1_rows = send1.reshape(num_cols, LANES)
    land1_rows = land1.reshape(num_mem * blk, LANES)
    send2_rows = send2.reshape(num_mem * blk, LANES)
    land2_rows = land2.reshape(num_cols, LANES)

    side = 4
    chip = me // 2
    z_at = [(chip // (side * side) + d) % side * (2 * side * side) for d in range(side)]
    y_at = [(chip // side % side + d) % side * (2 * side) for d in range(side)]
    x_at = [(chip % side + d) % side * 2 for d in range(side)]
    c_at = [(me + d) % 2 for d in range(2)]

    def scatter(src, dst, ss, rs):
        for dz, dy, dx, dc in far_first(side):
            peer = z_at[dz] + y_at[dy] + x_at[dx] + c_at[dc]
            pltpu.make_async_remote_copy(src_ref=src.at[peer, pl.ds(0, rows)], dst_ref=dst.at[me, pl.ds(0, rows)], send_sem=ss, recv_sem=rs,
                                         device_id={'ens': peer}, device_id_type=MESH).start()
        dst[pl.ds(me, 1), :rows] = src[pl.ds(me, 1), :rows]

    def settle(src, dst, ss, rs):
        sent = src.at[pl.ds(0, num_dev - 1), pl.ds(0, rows)]
        landed = dst.at[pl.ds(0, num_dev - 1), pl.ds(0, rows)]
        pltpu.make_async_copy(sent, landed, ss).wait()
        pltpu.make_async_copy(sent, landed, rs).wait()

    def place_lanes():
        wide[...] = jnp.zeros_like(wide)
        for j in range(blk):
            wide[j, :num_cycles, :num_obs] = y_in[:, j, :]
        for o in range(2 * halo + 1):
            wide[blk + o, :blk, :num_obs] = r_in[o]
        full = wide[0]
        for j in range(1, blk):
            full = full + pltpu.roll(wide[j], j * num_obs, 1)
        y_ref[...] = full[:num_cycles]
        row = lax.broadcasted_iota(jnp.int32, (8, LANES), 0)
        full = jnp.zeros((8, LANES), F32)
        for j in range(blk):
            for o in range(2 * halo + 1):
                at = window_lane(j + o - halo, blk, num_obs)
                moved = wide[blk + o] if at == 0 else pltpu.roll(wide[blk + o], at, 1)
                full = full + jnp.where(row == j, moved, 0.0)
        r_ref[...] = full
    place_lanes()

    def y_copies():
        right = lax.rem(me + 1, num_dev)
        left = lax.rem(me + num_dev - 1, num_dev)
        return (pltpu.make_async_remote_copy(src_ref=y_ref, dst_ref=yprev, send_sem=sy0, recv_sem=ry0,
                                             device_id={'ens': right}, device_id_type=MESH),
                pltpu.make_async_remote_copy(src_ref=y_ref, dst_ref=ynext, send_sem=sy1, recv_sem=ry1,
                                             device_id={'ens': left}, device_id_type=MESH))

    TILE = 256
    def forecast():
        for l in range(num_layers):
            mixed = dot32(state[...].astype(BF16), mix_s[...]).astype(BF16)
            mixed = jnp.concatenate([mixed, jnp.zeros((LANES - ROWS, num_cols), BF16)], axis=0)
            acts = []
            for c in range(num_cols // TILE):
                hidden = []
                for t in range(win_s.shape[1] // TILE):
                    half = dot32(win_s[l, pl.ds(t * TILE, TILE), :], mixed[:, c * TILE:(c + 1) * TILE])
                    hidden.append(gelu_of_double(half).astype(BF16))
                acts.append(jnp.concatenate(hidden, axis=0))
            for c in range(num_cols // TILE):
                state[:, c * TILE:(c + 1) * TILE] += dot32(wout_s[l], acts[c])

    own_col = lax.broadcasted_iota(jnp.int32, (PART, num_cols), 1) % blk

    def pack_state():
        obs = state[:num_obs, :]
        spread = jnp.zeros((PART, num_cols), F32)
        for j in range(rows):
            part = state[j * PART:(j + 1) * PART, :]
            spread = jnp.where(own_col == j, pltpu.roll(part, num_cols - (rows - j), 1), spread)
        send1_rows[...] = jnp.concatenate([
            state[:PART_LANE, :], spread, pltpu.roll(obs, rows, 1), pltpu.roll(obs, num_cols - blk, 1),
            jnp.zeros((LANES - HALO_LANE - 2 * num_obs, num_cols), F32)], axis=0).T

    def unpack_state():
        landed = land2_rows[...].T
        spread = landed[PART_LANE:HALO_LANE]
        for j in range(rows):
            part = landed[j * PART:(j + 1) * PART]
            state[j * PART:(j + 1) * PART, :] = jnp.where(own_col == rows, pltpu.roll(spread, rows - j, 1), part)

    mem_lane = lax.broadcasted_iota(jnp.int32, (num_mem, LANES), 1)

    def analyse(cycle):
        raws = [land1_rows[pl.ds(j, num_mem, stride=blk), :] for j in range(rows)]
        def moved(j, by):
            return pltpu.roll(raws[j], by % LANES, 1)
        second = moved(1, PART - PART_LANE)
        last = jnp.where(mem_lane < PART, moved(0, -PART_LANE), second)
        last = jnp.where(mem_lane < 2 * PART, last, moved(2, 2 * PART - PART_LANE))
        first_halo = blk * num_obs
        pieces = [raws[0], moved(1, num_obs), moved(2, 2 * num_obs), moved(0, 3 * num_obs - PART_LANE),
                  moved(0, first_halo - HALO_LANE), second, moved(2, first_halo + 4 * num_obs - HALO_LANE)]
        ends = [num_obs, 2 * num_obs, 3 * num_obs, 4 * num_obs, 6 * num_obs, 8 * num_obs, 10 * num_obs]
        obs_raw = jnp.zeros((num_mem, LANES), F32)
        for piece, end in reversed(list(zip(pieces, ends))):
            obs_raw = jnp.where(mem_lane < end, piece, obs_raw)
        raws.append(last)
        obs_mean = jnp.mean(obs_raw, axis=0, keepdims=True)
        pert = obs_raw - obs_mean
        innov = yall[pl.ds(cycle, 1), :] - obs_mean
        r_all = r_ref[:blk, :]
        energy = jnp.sum(pert * pert, axis=0, keepdims=True)
        base = (num_mem - 1) / INFLATION
        trace = num_mem * base + jnp.sum(r_all * energy, axis=1, keepdims=True)
        innov_rows = jnp.where(lax.broadcasted_iota(jnp.int32, (LANES, LANES), 0) == GAIN_LANE, innov, 0.0)
        right = jnp.concatenate([pert, innov_rows], axis=0)
        means, xs, zs = [], [], []
        threehalf = 1.5 * eye
        right = rhs_pack(right.T)
        for j in range(blk):
            res = dot32(lhs_pack(pert * r_all[j:j + 1]), right)
            inv = 1.0 / trace[j:j + 1]
            xs.append((res[:, :LANES] + base * eye) * (0.5 * inv))
            mean = jnp.mean(raws[j], axis=0, keepdims=True)
            means.append(mean)
            zs.append(jnp.where(mem_lane < num_vars, raws[j] - mean, res[:, LANES:]))

        for _ in range(NS_STEPS - 1):
            pairs, firsts = [], []
            for j in range(blk):
                hi, mid, lo = split3(threehalf - xs[j])
                res = dot32(jnp.concatenate([hi, mid, hi, mid, hi, lo], axis=1),
                            rhs_pack(jnp.concatenate([xs[j], zs[j]], axis=1)))
                firsts.append(res[:, :LANES])
                zs[j] = res[:, LANES:]
                both = jnp.concatenate([hi, mid], axis=1)
                pairs.append((jnp.concatenate([both, both], axis=0), jnp.concatenate([lo, hi], axis=0)))
            for j in range(blk):
                hi, mid, lo = split3(firsts[j])
                wide = dot32(jnp.concatenate([hi, mid], axis=1), pairs[j][0])
                thin = dot32(jnp.concatenate([hi, lo], axis=1), pairs[j][1])
                xs[j] = wide[:, :LANES] + (wide[:, LANES:] + thin)

        fins = [None] * blk
        for j in [rows, *range(rows)]:
            fins[j] = dot32(lhs_pack(threehalf - xs[j]), rhs_pack(zs[j]))
        spread = None
        for j in [rows, *range(rows)]:
            fin = fins[j]
            inv = 1.0 / trace[j:j + 1]
            shift = jnp.sum(fin * fin[:, GAIN_LANE:GAIN_LANE + 1], axis=0, keepdims=True) * inv
            new = means[j] + shift + (math.sqrt(num_mem - 1) * jnp.sqrt(inv)) * fin
            new = jnp.where(mem_lane < num_vars, new, 0.0)
            if j == rows:
                spread = [pltpu.roll(new, PART_LANE - n * PART, 1) for n in range(rows)]
            else:
                send2_rows[pl.ds(j, num_mem, stride=blk), :] = jnp.where(mem_lane < PART_LANE, new, spread[j])

    def cycle_body(cycle, carry):
        forecast()
        @pl.when(cycle == 0)
        def _():
            pl.semaphore_wait(bar, num_dev - 1)
            for copy in y_copies():
                copy.start()
        pack_state()
        scatter(send1, land1, s1, r1)
        @pl.when(cycle == 0)
        def _():
            for copy in y_copies():
                copy.wait()
            ylane = lax.broadcasted_iota(jnp.int32, (num_cycles, LANES), 1)
            full = y_ref[...]
            for n in range(halo):
                for col, src, at in ((n - halo, yprev, blk - halo + n), (blk + n, ynext, n)):
                    to = window_lane(col, blk, num_obs)
                    here = (ylane >= to) & (ylane < to + num_obs)
                    full = jnp.where(here, pltpu.roll(src[...], (to - at * num_obs) % LANES, 1), full)
            yall[...] = full
        settle(send1, land1, s1, r1)
        analyse(cycle)
        scatter(send2, land2, s2, r2)
        settle(send2, land2, s2, r2)
        unpack_state()
        return carry
    lax.fori_loop(0, num_cycles, cycle_body, 0)

    out_ref[:, 0, :] = jnp.dot(var_slot[:, :ROWS], state[...], precision=FULL, preferred_element_type=F32)


def solution(mesh):
    num_dev = mesh.shape['ens']

    def local_run(x_blk, a_mix, w_in, w_out, y_blk, r_blk, obs_idx):
        _, num_cols, num_vars = x_blk.shape
        num_cycles, blk, num_obs = y_blk.shape
        halo = (r_blk.shape[1] - 1) // 2
        num_layers, _, num_hid = w_in.shape
        vmem = pl.BlockSpec(memory_space=pltpu.VMEM)
        block = pltpu.VMEM((num_dev, blk, LANES), F32)
        out = pl.pallas_call(
            functools.partial(kernel, num_dev, num_cycles, num_obs, halo),
            out_shape=jax.ShapeDtypeStruct((num_vars, 1, num_cols), F32),
            in_specs=[pl.BlockSpec(memory_space=pltpu.SMEM)] + [vmem] * 6,
            out_specs=vmem,
            scratch_shapes=[
                pltpu.VMEM((ROWS, num_cols), F32),
                pltpu.VMEM((num_cols, num_cols), BF16),
                pltpu.VMEM((num_layers, num_hid, LANES), BF16),
                pltpu.VMEM((num_layers, ROWS, num_hid), BF16),
                block, block, block, block,
                pltpu.VMEM((num_cycles, LANES), F32),
                pltpu.VMEM((num_cycles, LANES), F32),
                pltpu.VMEM((num_cycles, LANES), F32),
                pltpu.VMEM((num_cycles, LANES), F32),
                pltpu.VMEM((blk + 2 * halo + 1, 8, LANES), F32),
                pltpu.VMEM((8, LANES), F32),
            ] + [pltpu.SemaphoreType.DMA] * 8,
            compiler_params=pltpu.CompilerParams(collective_id=0, has_side_effects=True),
        )(obs_idx, jnp.transpose(x_blk, (2, 0, 1)), a_mix, jnp.swapaxes(w_in, 1, 2), jnp.swapaxes(w_out, 1, 2), y_blk, jnp.swapaxes(r_blk, 0, 1))
        return jnp.transpose(out, (1, 2, 0))

    row_spec = P(('case', 'ens'), None, None)
    return jax.shard_map(local_run, mesh=mesh,
                         in_specs=(row_spec, P(), P(), P(), P(None, ('case', 'ens'), None), row_spec, P()),
                         out_specs=row_spec, check_vma=False)
```

```python
import functools
import math
import random
import jax
import jax.numpy as jnp
from jax import lax
from jax.experimental import pallas as pl
from jax.experimental.pallas import tpu as pltpu
from jax.sharding import PartitionSpec as P

INFLATION = 1.2
NS_STEPS = 16
FULL = lax.Precision.HIGHEST
MESH = pl.DeviceIdType.MESH
BF16 = jnp.bfloat16
F32 = jnp.float32
LANES = 128
PART = 24
PART_LANE = 3 * PART
HALO_LANE = 4 * PART
GAIN_LANE = 127
ROWS = 80


def split3(x):
    hi = x.astype(BF16)
    rest = x - hi.astype(F32)
    mid = rest.astype(BF16)
    lo = (rest - mid.astype(F32)).astype(BF16)
    return hi, mid, lo


def lhs_pack(x):
    hi, mid, lo = split3(x)
    return jnp.concatenate([hi, mid, hi, mid, hi, lo], axis=1)


def rhs_pack(x):
    hi, mid, lo = split3(x)
    return jnp.concatenate([hi, hi, mid, mid, lo, hi], axis=0)


def window_lane(col, blk, num_obs):
    if col < 0:
        return (blk + 2 * (col + blk - 1)) * num_obs
    if col < blk:
        return col * num_obs
    return (blk + 2 * (col - blk) + 1) * num_obs


def far_first(side):
    offsets = [(z, y, x, c) for z in range(side) for y in range(side) for x in range(side) for c in range(2)][1:]
    random.Random(1).shuffle(offsets)
    return sorted(offsets, key=lambda o: -sum(min(d, side - d) for d in o[:3]))


def gelu_of_double(u):
    scale = math.sqrt(2 / math.pi)
    return u + u * jnp.tanh(u * (2 * scale + (8 * scale * 0.044715) * (u * u)))


def dot32(lhs, rhs):
    return jnp.dot(lhs, rhs, preferred_element_type=F32)


def kernel(num_dev, num_cycles, num_obs, halo,
           obs_ref, x_ref, a_ref, win_ref, wout_ref, y_in, r_in,
           out_ref,
           state, mix_s, win_s, wout_s, send1, land1, send2, land2, y_ref, yprev, ynext, yall, wide, r_ref,
           s1, r1, s2, r2, sy0, ry0, sy1, ry1):
    me = lax.axis_index('ens')
    num_vars, _, num_cols = x_ref.shape
    num_layers = win_ref.shape[0]
    blk = num_cols // num_dev
    num_mem = num_dev
    rows = blk - 1
    land2[:, rows:, :] = jnp.zeros((num_cols // blk, 1, LANES), F32)

    bar = pltpu.get_barrier_semaphore()
    def greet(i, carry):
        pl.semaphore_signal(bar, inc=1, device_id={'ens': lax.rem(me + i, num_dev)}, device_id_type=MESH)
        return carry
    lax.fori_loop(1, num_dev, greet, 0)

    def order(dim):
        var = lax.broadcasted_iota(jnp.int32, (LANES, LANES), dim)
        slot = lax.broadcasted_iota(jnp.int32, (LANES, LANES), 1 - dim)
        place = var + num_obs
        for i in range(num_obs):
            place = place - jnp.where(var > obs_ref[i], 1, 0)
        for i in range(num_obs):
            place = jnp.where(var == obs_ref[i], i, place)
        return jnp.where((place == slot) & (var < num_vars), 1.0, 0.0).astype(F32)
    var_slot = order(0)[:num_vars]
    slot_var = order(1)[:, :num_vars]
    eye = jnp.where(lax.broadcasted_iota(jnp.int32, (LANES, LANES), 0)
                    == lax.broadcasted_iota(jnp.int32, (LANES, LANES), 1), 1.0, 0.0).astype(F32)
    eye_cols = jnp.where(lax.broadcasted_iota(jnp.int32, (num_cols, num_cols), 0)
                         == lax.broadcasted_iota(jnp.int32, (num_cols, num_cols), 1), 1.0, 0.0).astype(BF16)

    state[...] = jnp.dot(slot_var[:ROWS], x_ref[:, 0, :], precision=FULL, preferred_element_type=F32)
    mix_s[...] = lax.dot_general(eye_cols, a_ref[...], (((1,), (1,)), ((), ())),
                                 preferred_element_type=F32).astype(BF16)
    for l in range(num_layers):
        win_s[l] = (0.5 * lax.dot_general(win_ref[l], var_slot.astype(BF16), (((0,), (0,)), ((), ())),
                                          preferred_element_type=F32)).astype(BF16)
        wout_s[l] = jnp.dot(slot_var[:ROWS].astype(BF16), wout_ref[l], preferred_element_type=F32).astype(BF16)

    send1_rows = send1.reshape(num_cols, LANES)
    land1_rows = land1.reshape(num_mem * blk, LANES)
    send2_rows = send2.reshape(num_mem * blk, LANES)
    land2_rows = land2.reshape(num_cols, LANES)

    side = 4
    chip = me // 2
    z_at = [(chip // (side * side) + d) % side * (2 * side * side) for d in range(side)]
    y_at = [(chip // side % side + d) % side * (2 * side) for d in range(side)]
    x_at = [(chip % side + d) % side * 2 for d in range(side)]
    c_at = [(me + d) % 2 for d in range(2)]

    def scatter(src, dst, ss, rs):
        for dz, dy, dx, dc in far_first(side):
            peer = z_at[dz] + y_at[dy] + x_at[dx] + c_at[dc]
            pltpu.make_async_remote_copy(src_ref=src.at[peer, pl.ds(0, rows)], dst_ref=dst.at[me, pl.ds(0, rows)], send_sem=ss, recv_sem=rs,
                                         device_id={'ens': peer}, device_id_type=MESH).start()
        dst[pl.ds(me, 1), :rows] = src[pl.ds(me, 1), :rows]

    def settle(src, dst, ss, rs):
        sent = src.at[pl.ds(0, num_dev - 1), pl.ds(0, rows)]
        landed = dst.at[pl.ds(0, num_dev - 1), pl.ds(0, rows)]
        pltpu.make_async_copy(sent, landed, ss).wait()
        pltpu.make_async_copy(sent, landed, rs).wait()

    def place_lanes():
        wide[...] = jnp.zeros_like(wide)
        for j in range(blk):
            wide[j, :num_cycles, :num_obs] = y_in[:, j, :]
        for o in range(2 * halo + 1):
            wide[blk + o, :blk, :num_obs] = r_in[o]
        full = wide[0]
        for j in range(1, blk):
            full = full + pltpu.roll(wide[j], j * num_obs, 1)
        y_ref[...] = full[:num_cycles]
        row = lax.broadcasted_iota(jnp.int32, (8, LANES), 0)
        full = jnp.zeros((8, LANES), F32)
        for j in range(blk):
            for o in range(2 * halo + 1):
                at = window_lane(j + o - halo, blk, num_obs)
                moved = wide[blk + o] if at == 0 else pltpu.roll(wide[blk + o], at, 1)
                full = full + jnp.where(row == j, moved, 0.0)
        r_ref[...] = full
    place_lanes()

    def y_copies():
        right = lax.rem(me + 1, num_dev)
        left = lax.rem(me + num_dev - 1, num_dev)
        return (pltpu.make_async_remote_copy(src_ref=y_ref, dst_ref=yprev, send_sem=sy0, recv_sem=ry0,
                                             device_id={'ens': right}, device_id_type=MESH),
                pltpu.make_async_remote_copy(src_ref=y_ref, dst_ref=ynext, send_sem=sy1, recv_sem=ry1,
                                             device_id={'ens': left}, device_id_type=MESH))

    TILE = 256
    def forecast():
        for l in range(num_layers):
            mixed = dot32(state[...].astype(BF16), mix_s[...]).astype(BF16)
            mixed = jnp.concatenate([mixed, jnp.zeros((LANES - ROWS, num_cols), BF16)], axis=0)
            acts = []
            for c in range(num_cols // TILE):
                hidden = []
                for t in range(win_s.shape[1] // TILE):
                    half = dot32(win_s[l, pl.ds(t * TILE, TILE), :], mixed[:, c * TILE:(c + 1) * TILE])
                    hidden.append(gelu_of_double(half).astype(BF16))
                acts.append(jnp.concatenate(hidden, axis=0))
            for c in range(num_cols // TILE):
                state[:, c * TILE:(c + 1) * TILE] += dot32(wout_s[l], acts[c])

    own_col = lax.broadcasted_iota(jnp.int32, (PART, num_cols), 1) % blk

    def pack_state():
        obs = state[:num_obs, :]
        spread = jnp.zeros((PART, num_cols), F32)
        for j in range(rows):
            part = state[j * PART:(j + 1) * PART, :]
            spread = jnp.where(own_col == j, pltpu.roll(part, num_cols - (rows - j), 1), spread)
        send1_rows[...] = jnp.concatenate([
            state[:PART_LANE, :], spread, pltpu.roll(obs, rows, 1), pltpu.roll(obs, num_cols - blk, 1),
            jnp.zeros((LANES - HALO_LANE - 2 * num_obs, num_cols), F32)], axis=0).T

    def unpack_state():
        landed = land2_rows[...].T
        spread = landed[PART_LANE:HALO_LANE]
        for j in range(rows):
            part = landed[j * PART:(j + 1) * PART]
            state[j * PART:(j + 1) * PART, :] = jnp.where(own_col == rows, pltpu.roll(spread, rows - j, 1), part)

    mem_lane = lax.broadcasted_iota(jnp.int32, (num_mem, LANES), 1)

    def analyse(cycle):
        raws = [land1_rows[pl.ds(j, num_mem, stride=blk), :] for j in range(rows)]
        def moved(j, by):
            return pltpu.roll(raws[j], by % LANES, 1)
        second = moved(1, PART - PART_LANE)
        last = jnp.where(mem_lane < PART, moved(0, -PART_LANE), second)
        last = jnp.where(mem_lane < 2 * PART, last, moved(2, 2 * PART - PART_LANE))
        first_halo = blk * num_obs
        pieces = [raws[0], moved(1, num_obs), moved(2, 2 * num_obs), moved(0, 3 * num_obs - PART_LANE),
                  moved(0, first_halo - HALO_LANE), second, moved(2, first_halo + 4 * num_obs - HALO_LANE)]
        ends = [num_obs, 2 * num_obs, 3 * num_obs, 4 * num_obs, 6 * num_obs, 8 * num_obs, 10 * num_obs]
        obs_raw = jnp.zeros((num_mem, LANES), F32)
        for piece, end in reversed(list(zip(pieces, ends))):
            obs_raw = jnp.where(mem_lane < end, piece, obs_raw)
        raws.append(last)
        obs_mean = jnp.mean(obs_raw, axis=0, keepdims=True)
        pert = obs_raw - obs_mean
        innov = yall[pl.ds(cycle, 1), :] - obs_mean
        r_all = r_ref[:blk, :]
        energy = jnp.sum(pert * pert, axis=0, keepdims=True)
        base = (num_mem - 1) / INFLATION
        trace = num_mem * base + jnp.sum(r_all * energy, axis=1, keepdims=True)
        innov_rows = jnp.where(lax.broadcasted_iota(jnp.int32, (LANES, LANES), 0) == GAIN_LANE, innov, 0.0)
        right = jnp.concatenate([pert, innov_rows], axis=0)
        means, xs, zs = [], [], []
        threehalf = 1.5 * eye
        right = rhs_pack(right.T)
        for j in range(blk):
            res = dot32(lhs_pack(pert * r_all[j:j + 1]), right)
            inv = 1.0 / trace[j:j + 1]
            xs.append((res[:, :LANES] + base * eye) * (0.5 * inv))
            mean = jnp.mean(raws[j], axis=0, keepdims=True)
            means.append(mean)
            zs.append(jnp.where(mem_lane < num_vars, raws[j] - mean, res[:, LANES:]))

        for _ in range(NS_STEPS - 1):
            pairs, firsts = [], []
            for j in range(blk):
                hi, mid, lo = split3(threehalf - xs[j])
                res = dot32(jnp.concatenate([hi, mid, hi, mid, hi, lo], axis=1),
                            rhs_pack(jnp.concatenate([xs[j], zs[j]], axis=1)))
                firsts.append(res[:, :LANES])
                zs[j] = res[:, LANES:]
                both = jnp.concatenate([hi, mid], axis=1)
                pairs.append((jnp.concatenate([both, both], axis=0), jnp.concatenate([lo, hi], axis=0)))
            for j in range(blk):
                hi, mid, lo = split3(firsts[j])
                wide = dot32(jnp.concatenate([hi, mid], axis=1), pairs[j][0])
                thin = dot32(jnp.concatenate([hi, lo], axis=1), pairs[j][1])
                xs[j] = wide[:, :LANES] + (wide[:, LANES:] + thin)

        fins = [None] * blk
        for j in [rows, *range(rows)]:
            fins[j] = dot32(lhs_pack(threehalf - xs[j]), rhs_pack(zs[j]))
        spread = None
        for j in [rows, *range(rows)]:
            fin = fins[j]
            inv = 1.0 / trace[j:j + 1]
            shift = jnp.sum(fin * fin[:, GAIN_LANE:GAIN_LANE + 1], axis=0, keepdims=True) * inv
            new = means[j] + shift + (math.sqrt(num_mem - 1) * jnp.sqrt(inv)) * fin
            new = jnp.where(mem_lane < num_vars, new, 0.0)
            if j == rows:
                spread = [pltpu.roll(new, PART_LANE - n * PART, 1) for n in range(rows)]
            else:
                send2_rows[pl.ds(j, num_mem, stride=blk), :] = jnp.where(mem_lane < PART_LANE, new, spread[j])

    def rest(cycle):
        analyse(cycle)
        scatter(send2, land2, s2, r2)
        settle(send2, land2, s2, r2)
        unpack_state()

    def cycle_body(cycle, carry):
        forecast()
        pack_state()
        scatter(send1, land1, s1, r1)
        settle(send1, land1, s1, r1)
        rest(cycle)
        return carry

    forecast()
    pl.semaphore_wait(bar, num_dev - 1)
    for copy in y_copies():
        copy.start()
    pack_state()
    scatter(send1, land1, s1, r1)
    for copy in y_copies():
        copy.wait()
    ylane = lax.broadcasted_iota(jnp.int32, (num_cycles, LANES), 1)
    full = y_ref[...]
    for n in range(halo):
        for col, src, at in ((n - halo, yprev, blk - halo + n), (blk + n, ynext, n)):
            to = window_lane(col, blk, num_obs)
            here = (ylane >= to) & (ylane < to + num_obs)
            full = jnp.where(here, pltpu.roll(src[...], (to - at * num_obs) % LANES, 1), full)
    yall[...] = full
    settle(send1, land1, s1, r1)
    rest(0)
    lax.fori_loop(1, num_cycles, cycle_body, 0)

    out_ref[:, 0, :] = jnp.dot(var_slot[:, :ROWS], state[...], precision=FULL, preferred_element_type=F32)


def solution(mesh):
    num_dev = mesh.shape['ens']

    def local_run(x_blk, a_mix, w_in, w_out, y_blk, r_blk, obs_idx):
        _, num_cols, num_vars = x_blk.shape
        num_cycles, blk, num_obs = y_blk.shape
        halo = (r_blk.shape[1] - 1) // 2
        num_layers, _, num_hid = w_in.shape
        vmem = pl.BlockSpec(memory_space=pltpu.VMEM)
        block = pltpu.VMEM((num_dev, blk, LANES), F32)
        out = pl.pallas_call(
            functools.partial(kernel, num_dev, num_cycles, num_obs, halo),
            out_shape=jax.ShapeDtypeStruct((num_vars, 1, num_cols), F32),
            in_specs=[pl.BlockSpec(memory_space=pltpu.SMEM)] + [vmem] * 6,
            out_specs=vmem,
            scratch_shapes=[
                pltpu.VMEM((ROWS, num_cols), F32),
                pltpu.VMEM((num_cols, num_cols), BF16),
                pltpu.VMEM((num_layers, num_hid, LANES), BF16),
                pltpu.VMEM((num_layers, ROWS, num_hid), BF16),
                block, block, block, block,
                pltpu.VMEM((num_cycles, LANES), F32),
                pltpu.VMEM((num_cycles, LANES), F32),
                pltpu.VMEM((num_cycles, LANES), F32),
                pltpu.VMEM((num_cycles, LANES), F32),
                pltpu.VMEM((blk + 2 * halo + 1, 8, LANES), F32),
                pltpu.VMEM((8, LANES), F32),
            ] + [pltpu.SemaphoreType.DMA] * 8,
            compiler_params=pltpu.CompilerParams(collective_id=0, has_side_effects=True),
        )(obs_idx, jnp.transpose(x_blk, (2, 0, 1)), a_mix, w_in, jnp.swapaxes(w_out, 1, 2), y_blk, jnp.swapaxes(r_blk, 0, 1))
        return jnp.transpose(out, (1, 2, 0))

    row_spec = P(('case', 'ens'), None, None)
    return jax.shard_map(local_run, mesh=mesh,
                         in_specs=(row_spec, P(), P(), P(), P(None, ('case', 'ens'), None), row_spec, P()),
                         out_specs=row_spec, check_vma=False)
```
